256 devices in a mesh: gx: 2 (over x_hi), gy: 2 (over core), gz: 64 (over z, y, x_lo).
Axes of the slice: x: 4 (x_hi: 2, x_lo: 2; x = x_hi * 2 + x_lo), y: 4, z: 8, core: 2. Of those that a mesh axis runs over, the one named last changes fastest.
Arguments:
- state: float32 [24, 32, 128, 512], P(None, 'gx', ('gy', 'gz')), may hold values from -6 to 6
- base: float32 [24, 32, 128, 512], P(None, 'gx', ('gy', 'gz')), may hold values from -0.6 to 0.6
- accum: float32 [24, 32, 128, 512], P(None, 'gx', ('gy', 'gz')), may hold values from -0.3 to 0.3
- owner: int32 [64], replicated, may hold values from 0 to 63, each once
Outputs:
- next_section: float32 [24, 32, 128, 512], P(None, 'gx', ('gy', 'gz'))
- accum_out: float32 [24, 32, 128, 512], P(None, 'gx', ('gy', 'gz'))
The draws below stay inside these ranges and needn't reach their ends.
Inputs may be any that keep to these rules, and one draw needn't show every extreme that they name: owner names every index of gz once.
All inputs are finite; a program needn't handle non-finite values.
Results may differ from the reference program's by a relative error of at most 0.00002.
Values sent between devices are 32-bit elements; how exact they have to be, the bound alone decides.
A program may use at most 192 MiB of HBM per device.

```python
import jax
import jax.numpy as jnp
from jax import lax

FIELDS = 24
BLOCK = 16
NX = 32
TILES = 128
TILE_CELLS = 512
N_GY = 2
N_GZ = 64


def block_scale(rng, shape, pieces, smallest, top_value):
    level, own = 1.0, jax.random.fold_in(rng, 6)
    for dim, blocks in pieces:
        draws = jnp.exp(jax.random.uniform(jax.random.fold_in(own, dim), (blocks,), jnp.float32, smallest / len(pieces), top_value / len(pieces)))
        level = level * jnp.repeat(draws, shape[dim] // blocks).reshape([-1 if axis == dim else 1 for axis in range(len(shape))])
    return level


def centred(own_key, shape, spread, bound, cuts=(), dtype=jnp.bfloat16):
    values = spread * jax.random.normal(own_key, shape, jnp.float32)
    if cuts:
        values = values * block_scale(own_key, shape, cuts, -0.22, 0.18)
    return jnp.clip(values, -bound, bound).astype(dtype)


def setup_inputs(seed: int = 0) -> dict:
    arg_keys = jax.random.split(jax.random.key(seed), 5)
    return {
        "state": centred(arg_keys[0], (FIELDS, NX, TILES, TILE_CELLS), 1.0, 6.0, ((1, 2), (2, 128)), jnp.float32),
        "base": centred(arg_keys[1], (FIELDS, NX, TILES, TILE_CELLS), 0.1, 0.6, ((1, 2), (2, 128)), jnp.float32),
        "accum": centred(arg_keys[2], (FIELDS, NX, TILES, TILE_CELLS), 0.05, 0.3, ((1, 2), (2, 128)), jnp.float32),
        "owner": jax.random.permutation(arg_keys[3], N_GZ).astype(jnp.int32),
    }


DAMPING_STRENGTH = 1.0
SPACING = 1.0
TIME_STEP = 0.25
SECTION_SHIFT = 0.5
SECTION_WEIGHT = 1.0 / 3.0


def shifted(padded, dimension, offset):
    selection = [slice(None)]
    for axis_index in range(1, 4):
        length = padded.shape[axis_index] - 6
        start_at = 3 + (offset if axis_index == dimension else 0)
        selection.append(slice(start_at, start_at + length))
    return padded[tuple(selection)]


def stencils(padded):
    laplace = 0.0
    damping = 0.0
    for dimension in (1, 2, 3):
        values = [shifted(padded, dimension, offset) for offset in range(-3, 4)]
        laplace = laplace + (-values[1] + 16.0 * values[2] - 30.0 * values[3] + 16.0 * values[4] - values[5]) / (12.0 * SPACING * SPACING)
        damping = damping + (values[0] - 6.0 * values[1] + 15.0 * values[2] - 20.0 * values[3] + 15.0 * values[4] - 6.0 * values[5] + values[6]) * (DAMPING_STRENGTH / (64.0 * SPACING))
    return laplace, damping


def rates_from(centre, laplace, damping):
    halves = centre.shape[0] // 2
    metric = centre[:halves]
    curvature = centre[halves:]
    lapse_value = 1.0 + 0.25 * jnp.tanh(metric[0])
    trace_value = jnp.mean(curvature, axis=0)
    metric_rate = -2.0 * lapse_value * curvature + damping[:halves]
    curvature_rate = -0.5 * lapse_value * laplace[:halves] + lapse_value * trace_value * curvature + damping[halves:]
    return jnp.concatenate([metric_rate, curvature_rate], axis=0)


def to_grid(stored, owner):
    fields = stored.shape[0]
    cells_x = stored.shape[1]
    side_y = BLOCK
    side_z = 2 * BLOCK
    blocked = stored.reshape(fields, cells_x, N_GY, N_GZ, side_y, side_z)
    ordered = jnp.take(blocked, owner, axis=3)
    whole_grid = ordered.transpose(0, 1, 2, 4, 3, 5)
    return whole_grid.reshape(fields, cells_x, N_GY * side_y, N_GZ * side_z)


def from_grid(whole_grid, owner):
    fields = whole_grid.shape[0]
    cells_x = whole_grid.shape[1]
    side_y = BLOCK
    side_z = 2 * BLOCK
    tiled = whole_grid.reshape(fields, cells_x, N_GY, side_y, N_GZ, side_z)
    tiled = tiled.transpose(0, 1, 2, 4, 3, 5)
    stored = jnp.zeros_like(tiled).at[:, :, :, owner].set(tiled)
    return stored.reshape(fields, cells_x, N_GY * N_GZ, side_y * side_z)


def per_field(single):
    laplace, damping = stencils(single[None])
    return laplace[0], damping[0]


def reference(state, base, accum, owner):
    whole_grid = to_grid(state, owner)
    padded = jnp.pad(whole_grid, ((0, 0), (3, 3), (3, 3), (3, 3)), mode="wrap")
    laplace, damping = lax.map(per_field, padded)
    rate_values = rates_from(whole_grid, laplace, damping)
    stored = from_grid(rate_values, owner)
    next_section = base + (SECTION_SHIFT * TIME_STEP) * stored
    accum_out = accum + (SECTION_WEIGHT * TIME_STEP) * stored
    return next_section, accum_out
```

```python
import functools

import jax
import jax.numpy as jnp
from jax import lax
from jax.experimental import pallas as pl
from jax.experimental.pallas import tpu as pltpu
from jax.sharding import PartitionSpec as P

MESH = pl.DeviceIdType.MESH
FIELDS, HALF = 24, 12
LANES = 128
C1 = 0.5 * 0.25
C2 = 0.25 / 3.0
DAMP = (-20.0 / 64.0, 15.0 / 64.0, -6.0 / 64.0, 1.0 / 64.0)
LAP = (-30.0 / 12.0, 16.0 / 12.0, -1.0 / 12.0)
MIDS = 40


def lane_iota(rows=8):
    return lax.broadcasted_iota(jnp.int32, (rows, LANES), 1)


def roll(v, s):
    s %= LANES
    return v if s == 0 else pltpu.roll(v, s, axis=1)


def mid_of(w, i):
    return lax.rem(i + 3 * w, 8)


def kernel_a(state, base, accum, owner, q1, q2, gb, lapse_out,
             xp, sy, bs, ac, rt, lap, mb, rb, fb, xs, xr, tabv, tab,
             s_in, s_tab, s_out, s_y, r_y, s_x, r_x, s_1, r_1, s_2, r_2, s_self):
    gx, gy, me = lax.axis_index("gx"), lax.axis_index("gy"), lax.axis_index("gz")
    z, w = me // 8, lax.rem(me, 8)
    mine = lax.rem(z + 40 - 3 * w - 4 * gy, 8)
    is_mid = mine < 5
    my_g = w * 5 + mine

    load_state = pltpu.make_async_copy(state, xp.at[:, pl.ds(16, 64)], s_in.at[0])
    load_base = pltpu.make_async_copy(base, bs, s_in.at[1])
    load_accum = pltpu.make_async_copy(accum, ac, s_in.at[2])
    load_state.start()
    load_base.start()
    load_accum.start()

    barrier = pltpu.get_barrier_semaphore()

    @pl.loop(1, 64)
    def _(k):
        pl.semaphore_signal(barrier, inc=1, device_id={"gz": lax.rem(me + k, 64)}, device_id_type=MESH)

    pl.semaphore_signal(barrier, inc=1, device_id={"gy": 1 - gy}, device_id_type=MESH)
    pl.semaphore_signal(barrier, inc=1, device_id={"gx": 1 - gx}, device_id_type=MESH)

    lanes = lane_iota()
    below = jnp.zeros((8, LANES), jnp.int32)
    above = jnp.zeros((8, LANES), jnp.int32)
    for c in range(64):
        hit = lanes == owner[c]
        below = jnp.where(hit, owner[(c + 63) % 64], below)
        above = jnp.where(hit, owner[(c + 1) % 64], above)
    tabv[0] = below
    tabv[1] = above
    load_tab = pltpu.make_async_copy(tabv, tab, s_tab)

    b = lanes % 32
    u = (lanes + 3) % 32
    load_state.wait()
    load_tab.start()

    def tile(f, xg, q):
        return xp[f, pl.ds(16 + xg * 32 + q, 8, stride=4), :]

    @pl.loop(0, 8)
    def _(g):
        for p in range(5):
            acc = jnp.zeros((8, LANES), jnp.float32)
            for r in range(5 if p < 4 else 4):
                n = p * 5 + r
                v = tile(g * 3 + n // 8, (n % 8) // 4, n % 4)
                x = jnp.where(b < 3, roll(v, 32), roll(v, 96))
                window = (u + 32 - 6 * r) % 32 < 6
                acc = jnp.where(window, roll(x, 6 * r), acc)
            mb[g * 5 + p] = acc

    first = lax.broadcasted_iota(jnp.int32, (8, LANES), 0) < 4
    for f in range(0, FIELDS, 2):
        lo0, lo1 = xp[f, pl.ds(24, 8), :], xp[f + 1, pl.ds(24, 8), :]
        hi0, hi1 = xp[f, pl.ds(64, 8), :], xp[f + 1, pl.ds(64, 8), :]
        xs[0, f // 2] = jnp.where(first, lo0, pltpu.roll(lo1, 4, axis=0))
        xs[1, f // 2] = jnp.where(first, pltpu.roll(hi0, 4, axis=0), hi1)

    pl.semaphore_wait(barrier, 65)

    def send_1(k):
        dw, i = k // 5, lax.rem(k + z, 5)
        ow = lax.rem(w + dw, 8)
        oz = lax.rem(i + 3 * ow + 4 * gy, 8)
        peer = oz * 8 + ow
        return peer, ow * 5 + i

    @pl.loop(0, MIDS)
    def _(k):
        peer, g = send_1(k)

        @pl.when(peer != me)
        def _():
            pltpu.make_async_remote_copy(
                mb.at[g], rb.at[me], s_1, r_1, device_id={"gz": peer}, device_id_type=MESH).start()

    send_y = pltpu.make_async_remote_copy(
        xp.at[:, pl.ds(16, 64)], sy, s_y, r_y, device_id={"gy": 1 - gy}, device_id_type=MESH)
    send_y.start()
    send_x = [
        pltpu.make_async_remote_copy(
            xp.at[:, pl.ds(16, 8)], xp.at[:, pl.ds(80, 8)], s_x.at[0], r_x.at[0],
            device_id={"gx": 1 - gx}, device_id_type=MESH),
        pltpu.make_async_remote_copy(
            xp.at[:, pl.ds(72, 8)], xp.at[:, pl.ds(8, 8)], s_x.at[1], r_x.at[1],
            device_id={"gx": 1 - gx}, device_id_type=MESH),
        pltpu.make_async_remote_copy(
            xs, xr, s_x.at[2], r_x.at[2], device_id={"gx": 1 - gx}, device_id_type=MESH),
    ]
    for s in send_x:
        s.start()

    @pl.when(is_mid)
    def _():
        rb[me] = mb[my_g]

    load_tab.wait()
    send_y.wait_recv()

    for t in range(8):
        xg, q = t // 4, t % 4
        lap[t] = 1.0 + 0.25 * jnp.tanh(tile(0, xg, q))
        total = tile(12, xg, q)
        for f in range(13, 24):
            total = total + tile(f, xg, q)
        lap[8 + t] = lap[t] * (total * (1.0 / 12.0))

    low = [b >= k for k in (1, 2, 3)]
    high = [b < 32 - k for k in (1, 2, 3)]
    left = [lanes >= 32 * k for k in (1, 2, 3)]
    right = [lanes < 128 - 32 * k for k in (1, 2, 3)]

    def plane(f, xg):
        values = [sy[f, pl.ds(xg * 32 + 3, 8, stride=4), :]]
        values += [tile(f, xg, q) for q in range(4)]
        values += [sy[f, pl.ds(xg * 32, 8, stride=4), :]]
        turned = [[v] + [roll(v, 32 * j) for j in (1, 2, 3)] for v in values]
        sums = []
        for q in range(4):
            v = values[q + 1]
            three = []
            for k in (1, 2, 3):
                plus = jnp.where(right[k - 1], turned[q + 1][4 - k], turned[q + 2][4 - k])
                minus = jnp.where(left[k - 1], turned[q + 1][k], turned[q][k])
                up = jnp.where(high[k - 1], roll(v, -k), 0.0)
                down = jnp.where(low[k - 1], roll(v, k), 0.0)
                three.append((plus + minus) + (up + down))
            sums.append((v, three))
        return sums

    @pl.loop(0, HALF)
    def _(f):
        for xg in range(2):
            us, vs = plane(f, xg), plane(f + HALF, xg)
            for q in range(4):
                t = xg * 4 + q
                lapse, drag = lap[t], lap[8 + t]
                uv, (u1, u2, u3) = us[q]
                vv, (v1, v2, v3) = vs[q]
                damp_u = (2 * DAMP[0]) * uv + DAMP[1] * u1 + DAMP[2] * u2 + DAMP[3] * u3
                damp_v = (2 * DAMP[0]) * vv + DAMP[1] * v1 + DAMP[2] * v2 + DAMP[3] * v3
                laplace = (2 * LAP[0]) * uv + LAP[1] * u1 + LAP[2] * u2
                rt[f, t] = damp_u - 2.0 * lapse * vv
                rt[f + HALF, t] = damp_v + drag * vv - 0.5 * lapse * laplace

    load_base.wait()
    load_accum.wait()

    @pl.when(is_mid)
    def _():
        pltpu.make_async_copy(rb.at[pl.ds(0, 63)], rb.at[pl.ds(0, 63)], r_1).wait()
        kind = (u < 30) & (lax.rem(u, 6) < 3)

        @pl.loop(0, 64, unroll=8)
        def _(g):
            fb[g] = jnp.where(kind, rb[tab[0, 0, g]], rb[tab[1, 0, g]])

        @pl.loop(1, 64)
        def _(k):
            peer = lax.rem(me + k, 64)
            pltpu.make_async_remote_copy(
                fb.at[peer], gb.at[my_g], s_2, r_2, device_id={"gz": peer}, device_id_type=MESH).start()

        pltpu.make_async_copy(fb.at[me], gb.at[my_g], s_self).start()

    for s in send_x:
        s.wait_recv()
    for f in range(0, FIELDS, 2):
        hi, lo = xr[0, f // 2], xr[1, f // 2]
        xp[f, pl.ds(88, 8), :] = hi
        xp[f + 1, pl.ds(88, 8), :] = pltpu.roll(hi, 4, axis=0)
        xp[f, pl.ds(0, 8), :] = pltpu.roll(lo, 4, axis=0)
        xp[f + 1, pl.ds(0, 8), :] = lo

    @pl.loop(0, HALF)
    def _(f):
        for t in range(8):
            xg, q = t // 4, t % 4

            def shifted(field, k):
                return xp[field, pl.ds(16 + xg * 32 + 4 * k + q, 8, stride=4), :]

            def three(field):
                return [shifted(field, k) + shifted(field, -k) for k in (1, 2, 3)]

            uv, vv = shifted(f, 0), shifted(f + HALF, 0)
            u1, u2, u3 = three(f)
            v1, v2, v3 = three(f + HALF)
            damp_u = DAMP[0] * uv + DAMP[1] * u1 + DAMP[2] * u2 + DAMP[3] * u3
            damp_v = DAMP[0] * vv + DAMP[1] * v1 + DAMP[2] * v2 + DAMP[3] * v3
            laplace = LAP[0] * uv + LAP[1] * u1 + LAP[2] * u2
            rate_u = rt[f, t] + damp_u
            rate_v = rt[f + HALF, t] + damp_v - 0.5 * lap[t] * laplace
            rows = pl.ds(xg * 32 + q, 8, stride=4)
            for field, rate in ((f, rate_u), (f + HALF, rate_v)):
                bs[field, rows, :] = bs[field, rows, :] + C1 * rate
                ac[field, rows, :] = ac[field, rows, :] + C2 * rate

    out_1 = pltpu.make_async_copy(bs, q1, s_out.at[0])
    out_2 = pltpu.make_async_copy(ac, q2, s_out.at[1])
    out_3 = pltpu.make_async_copy(lap.at[pl.ds(0, 8)], lapse_out, s_out.at[2])
    out_1.start()
    out_2.start()
    out_3.start()
    send_y.wait_send()
    for s in send_x:
        s.wait_send()
    out_1.wait()
    out_2.wait()
    out_3.wait()

    @pl.when(is_mid)
    def _():
        pltpu.make_async_copy(mb.at[pl.ds(0, 39)], mb.at[pl.ds(0, 39)], s_1).wait()
        pltpu.make_async_copy(fb.at[pl.ds(0, 63)], fb.at[pl.ds(0, 63)], s_2).wait()
        pltpu.make_async_copy(fb.at[0], gb.at[0], s_self).wait()
        pltpu.make_async_copy(gb.at[pl.ds(0, 39)], gb.at[pl.ds(0, 39)], r_2).wait()

    @pl.when(jnp.logical_not(is_mid))
    def _():
        pltpu.make_async_copy(mb, mb, s_1).wait()
        pltpu.make_async_copy(gb, gb, r_2).wait()


def kernel_b(q1, q2, gb, lapse, o1, o2):
    b = lane_iota() % 32
    zero = jnp.zeros((8, LANES), jnp.float32)
    ups = [jnp.where(b >= 32 - k, 1.0, zero) for k in (1, 2, 3)]
    downs = [jnp.where(b < k, 1.0, zero) for k in (1, 2, 3)]
    for n in range(24):
        p, r = n // 5, n % 5
        t = n % 8
        xg, q = t // 4, t % 4
        rows = pl.ds(xg * 32 + q, 8, stride=4)

        def three(half):
            v = gb[half, 0, p]
            return [roll(v, -6 * r - k) * ups[k - 1] + roll(v, -6 * r + k) * downs[k - 1] for k in (1, 2, 3)]

        u1, u2, u3 = three(0)
        v1, v2, v3 = three(1)
        rate_u = DAMP[1] * u1 + DAMP[2] * u2 + DAMP[3] * u3
        rate_v = DAMP[1] * v1 + DAMP[2] * v2 + DAMP[3] * v3 - 0.5 * lapse[t] * (LAP[1] * u1 + LAP[2] * u2)
        for half, rate in ((0, rate_u), (1, rate_v)):
            o1[half, n // 8, rows, :] = q1[half, n // 8, rows, :] + C1 * rate
            o2[half, n // 8, rows, :] = q2[half, n // 8, rows, :] + C2 * rate


def local(state, base, accum, owner):
    shape = state.shape
    f32 = jnp.float32
    rows = (FIELDS, 64, LANES)
    any_spec = pl.BlockSpec(memory_space=pl.ANY)
    dma = pltpu.SemaphoreType.DMA
    q1, q2, gb, lapse = pl.pallas_call(
        kernel_a,
        out_shape=(
            jax.ShapeDtypeStruct(rows, f32),
            jax.ShapeDtypeStruct(rows, f32),
            jax.ShapeDtypeStruct((MIDS, 8, LANES), f32),
            jax.ShapeDtypeStruct((8, 8, LANES), f32),
        ),
        in_specs=[any_spec, any_spec, any_spec, pl.BlockSpec(memory_space=pltpu.SMEM)],
        out_specs=(any_spec,) * 4,
        scratch_shapes=[
            pltpu.VMEM((FIELDS, 96, LANES), f32),
            pltpu.VMEM(rows, f32),
            pltpu.VMEM(rows, f32),
            pltpu.VMEM(rows, f32),
            pltpu.VMEM((FIELDS, 8, 8, LANES), f32),
            pltpu.VMEM((16, 8, LANES), f32),
            pltpu.VMEM((MIDS, 8, LANES), f32),
            pltpu.VMEM((64, 8, LANES), f32),
            pltpu.VMEM((64, 8, LANES), f32),
            pltpu.VMEM((2, 12, 8, LANES), f32),
            pltpu.VMEM((2, 12, 8, LANES), f32),
            pltpu.VMEM((2, 8, LANES), jnp.int32),
            pltpu.SMEM((2, 8, LANES), jnp.int32),
            dma((3,)), dma, dma((3,)), dma, dma, dma((3,)), dma((3,)), dma, dma, dma, dma, dma,
        ],
        compiler_params=pltpu.CompilerParams(collective_id=0, has_side_effects=True, vmem_limit_bytes=24 << 20),
    )(state.reshape(rows), base.reshape(rows), accum.reshape(rows), owner)
    split = (2, HALF, 64, LANES)
    block = pl.BlockSpec((2, 3, 64, LANES), lambda i: (0, i, 0, 0))
    o1, o2 = pl.pallas_call(
        kernel_b,
        grid=(4,),
        out_shape=(jax.ShapeDtypeStruct(split, f32),) * 2,
        in_specs=[block, block,
                  pl.BlockSpec((2, 1, 5, 8, LANES), lambda i: (0, i, 0, 0, 0)),
                  pl.BlockSpec((8, 8, LANES), lambda i: (0, 0, 0))],
        out_specs=(block, block),
        compiler_params=pltpu.CompilerParams(dimension_semantics=("arbitrary",), vmem_limit_bytes=24 << 20),
    )(q1.reshape(split), q2.reshape(split), gb.reshape(2, 4, 5, 8, LANES), lapse)
    return o1.reshape(shape), o2.reshape(shape)


def solution(mesh):
    spec = P(None, "gx", ("gy", "gz"), None)
    return jax.shard_map(
        local, mesh=mesh, in_specs=(spec, spec, spec, P()), out_specs=(spec, spec), check_vma=False)
```

```python
import functools

import jax
import jax.numpy as jnp
from jax import lax
from jax.experimental import pallas as pl
from jax.experimental.pallas import tpu as pltpu
from jax.sharding import PartitionSpec as P

MESH = pl.DeviceIdType.MESH
FIELDS, HALF = 24, 12
LANES = 128
C1 = 0.5 * 0.25
C2 = 0.25 / 3.0
DAMP = (-20.0 / 64.0, 15.0 / 64.0, -6.0 / 64.0, 1.0 / 64.0)
LAP = (-30.0 / 12.0, 16.0 / 12.0, -1.0 / 12.0)
FAR_FIRST = (4, 3, 5, 2, 6, 1, 7, 0)


def lane_iota(rows=8):
    return lax.broadcasted_iota(jnp.int32, (rows, LANES), 1)


def roll(v, s):
    s %= LANES
    return v if s == 0 else pltpu.roll(v, s, axis=1)


def kernel_a(state, base, accum, owner_hbm, q1, q2,
             xp, sy, rt, lap, mb, rb, fb, gb, xs, xr, tabv, tab, owner,
             s_in, s_tab, s_y, r_y, s_x, r_x, s_1, r_1, s_2, r_2):
    gx, gy, me = lax.axis_index("gx"), lax.axis_index("gy"), lax.axis_index("gz")
    z, w = me // 8, lax.rem(me, 8)

    load_state = pltpu.make_async_copy(state, xp.at[:, pl.ds(16, 64)], s_in.at[0])
    load_base = pltpu.make_async_copy(base, q1, s_in.at[1])
    load_accum = pltpu.make_async_copy(accum, q2, s_in.at[2])
    load_owner = pltpu.make_async_copy(owner_hbm, owner, s_in.at[3])
    load_state.start()
    load_owner.start()

    barrier = pltpu.get_barrier_semaphore()

    @pl.loop(1, 64)
    def _(k):
        pl.semaphore_signal(barrier, inc=1, device_id={"gz": lax.rem(me + k, 64)}, device_id_type=MESH)

    pl.semaphore_signal(barrier, inc=1, device_id={"gy": 1 - gy}, device_id_type=MESH)
    pl.semaphore_signal(barrier, inc=1, device_id={"gx": 1 - gx}, device_id_type=MESH)
    load_base.start()
    load_accum.start()

    load_owner.wait()
    lanes = lane_iota()
    below = jnp.zeros((8, LANES), jnp.int32)
    above = jnp.zeros((8, LANES), jnp.int32)
    for c in range(64):
        hit = lanes == owner[c]
        below = jnp.where(hit, owner[(c + 63) % 64], below)
        above = jnp.where(hit, owner[(c + 1) % 64], above)
    tabv[0] = below
    tabv[1] = above
    load_tab = pltpu.make_async_copy(tabv, tab, s_tab)

    b = lanes % 32
    u = (lanes + 3) % 32
    load_state.wait()
    load_tab.start()

    def row(t):
        return (t // 4) * 32 + t % 4

    def tile(f, t):
        return xp[f, pl.ds(16 + row(t), 8, stride=4), :]

    @pl.loop(0, 8)
    def _(t):
        for p in range(5):
            acc = jnp.zeros((8, LANES), jnp.float32)
            for r in range(5 if p < 4 else 4):
                v = tile(p * 5 + r, t)
                x = jnp.where(b < 3, roll(v, 32), roll(v, 96))
                window = (u + 32 - 6 * r) % 32 < 6
                acc = jnp.where(window, roll(x, 6 * r), acc)
            mb[pl.ds(t * 64 + p, 8, stride=8), :] = acc

    first = lax.broadcasted_iota(jnp.int32, (8, LANES), 0) < 4
    for f in range(0, FIELDS, 2):
        lo0, lo1 = xp[f, pl.ds(24, 8), :], xp[f + 1, pl.ds(24, 8), :]
        hi0, hi1 = xp[f, pl.ds(64, 8), :], xp[f + 1, pl.ds(64, 8), :]
        xs[0, f // 2] = jnp.where(first, lo0, pltpu.roll(lo1, 4, axis=0))
        xs[1, f // 2] = jnp.where(first, pltpu.roll(hi0, 4, axis=0), hi1)

    pl.semaphore_wait(barrier, 65)

    def five(ref, j):
        if ref.shape[0] == 64:
            return ref.at[j, pl.ds(0, 5)]
        return ref.at[pl.ds(pl.multiple_of(8 * j, 8), 5)]

    def spread(source, target, send, recv):
        for d in FAR_FIRST:
            @pl.loop(0, 8)
            def _(k):
                peer = lax.rem(z + d, 8) * 8 + lax.rem(w + k, 8)

                @pl.when(peer != me)
                def _():
                    pltpu.make_async_remote_copy(
                        five(source, peer), five(target, me), send, recv,
                        device_id={"gz": peer}, device_id_type=MESH).start()

        pltpu.make_async_copy(five(source, me), five(target, me), recv).start()

    spread(mb, rb, s_1, r_1)

    send_y = pltpu.make_async_remote_copy(
        xp.at[:, pl.ds(16, 64)], sy, s_y, r_y, device_id={"gy": 1 - gy}, device_id_type=MESH)
    send_y.start()
    send_x = [
        pltpu.make_async_remote_copy(
            xp.at[:, pl.ds(16, 8)], xp.at[:, pl.ds(80, 8)], s_x.at[0], r_x.at[0],
            device_id={"gx": 1 - gx}, device_id_type=MESH),
        pltpu.make_async_remote_copy(
            xp.at[:, pl.ds(72, 8)], xp.at[:, pl.ds(8, 8)], s_x.at[1], r_x.at[1],
            device_id={"gx": 1 - gx}, device_id_type=MESH),
        pltpu.make_async_remote_copy(
            xs, xr, s_x.at[2], r_x.at[2], device_id={"gx": 1 - gx}, device_id_type=MESH),
    ]
    for s in send_x:
        s.start()

    load_tab.wait()
    for t in range(8):
        lap[t] = 1.0 + 0.25 * jnp.tanh(tile(0, t))
        total = tile(12, t)
        for f in range(13, 24):
            total = total + tile(f, t)
        lap[8 + t] = lap[t] * (total * (1.0 / 12.0))

    low = [b >= k for k in (1, 2, 3)]
    high = [b < 32 - k for k in (1, 2, 3)]
    left = [lanes >= 32 * k for k in (1, 2, 3)]
    right = [lanes < 128 - 32 * k for k in (1, 2, 3)]

    def plane(f, xg):
        values = [sy[f, pl.ds(xg * 32 + 3, 8, stride=4), :]]
        values += [tile(f, xg * 4 + q) for q in range(4)]
        values += [sy[f, pl.ds(xg * 32, 8, stride=4), :]]
        turned = [[v] + [roll(v, 32 * j) for j in (1, 2, 3)] for v in values]
        sums = []
        for q in range(4):
            v = values[q + 1]
            three = []
            for k in (1, 2, 3):
                plus = jnp.where(right[k - 1], turned[q + 1][4 - k], turned[q + 2][4 - k])
                minus = jnp.where(left[k - 1], turned[q + 1][k], turned[q][k])
                up = jnp.where(high[k - 1], roll(v, -k), 0.0)
                down = jnp.where(low[k - 1], roll(v, k), 0.0)
                three.append((plus + minus) + (up + down))
            sums.append((v, three))
        return sums

    send_y.wait_recv()

    @pl.loop(0, HALF)
    def _(f):
        for xg in range(2):
            us, vs = plane(f, xg), plane(f + HALF, xg)
            for q in range(4):
                t = xg * 4 + q
                lapse, drag = lap[t], lap[8 + t]
                uv, (u1, u2, u3) = us[q]
                vv, (v1, v2, v3) = vs[q]
                damp_u = (2 * DAMP[0]) * uv + DAMP[1] * u1 + DAMP[2] * u2 + DAMP[3] * u3
                damp_v = (2 * DAMP[0]) * vv + DAMP[1] * v1 + DAMP[2] * v2 + DAMP[3] * v3
                laplace = (2 * LAP[0]) * uv + LAP[1] * u1 + LAP[2] * u2
                rt[f, t] = damp_u - 2.0 * lapse * vv
                rt[f + HALF, t] = damp_v + drag * vv - 0.5 * lapse * laplace

    load_base.wait()
    load_accum.wait()
    pltpu.make_async_copy(rb.at[pl.ds(0, 40)], rb.at[pl.ds(0, 40)], r_1).wait()
    kind = (u < 30) & (lax.rem(u, 6) < 3)

    @pl.loop(0, 64, unroll=8)
    def _(g):
        fb[g] = jnp.where(kind, rb[tab[0, 0, g]], rb[tab[1, 0, g]])

    spread(fb, gb, s_2, r_2.at[z])

    for s in send_x:
        s.wait_recv()
    for f in range(0, FIELDS, 2):
        hi, lo = xr[0, f // 2], xr[1, f // 2]
        xp[f, pl.ds(88, 8), :] = hi
        xp[f + 1, pl.ds(88, 8), :] = pltpu.roll(hi, 4, axis=0)
        xp[f, pl.ds(0, 8), :] = pltpu.roll(lo, 4, axis=0)
        xp[f + 1, pl.ds(0, 8), :] = lo

    def add(f, t, rate):
        rows = pl.ds(row(t), 8, stride=4)
        q1[f, rows, :] = q1[f, rows, :] + C1 * rate
        q2[f, rows, :] = q2[f, rows, :] + C2 * rate

    @pl.loop(0, HALF)
    def _(f):
        for t in range(8):
            def shifted(field, k):
                return xp[field, pl.ds(16 + row(t) + 4 * k, 8, stride=4), :]

            def three(field):
                return [shifted(field, k) + shifted(field, -k) for k in (1, 2, 3)]

            uv, vv = shifted(f, 0), shifted(f + HALF, 0)
            u1, u2, u3 = three(f)
            v1, v2, v3 = three(f + HALF)
            damp_u = DAMP[0] * uv + DAMP[1] * u1 + DAMP[2] * u2 + DAMP[3] * u3
            damp_v = DAMP[0] * vv + DAMP[1] * v1 + DAMP[2] * v2 + DAMP[3] * v3
            laplace = LAP[0] * uv + LAP[1] * u1 + LAP[2] * u2
            add(f, t, rt[f, t] + damp_u)
            add(f + HALF, t, rt[f + HALF, t] + damp_v - 0.5 * lap[t] * laplace)

    send_y.wait_send()
    for s in send_x:
        s.wait_send()
    everything = pltpu.make_async_copy(mb.at[pl.ds(0, 315)], mb.at[pl.ds(0, 315)], s_1)
    everything.wait()

    zero = jnp.zeros((8, LANES), jnp.float32)
    ups = [jnp.where(b >= 32 - k, 1.0, zero) for k in (1, 2, 3)]
    downs = [jnp.where(b < k, 1.0, zero) for k in (1, 2, 3)]

    @pl.loop(0, 8)
    def _(k):
        near = lax.rem(k, 2) * ((k + 1) // 2) + (1 - lax.rem(k, 2)) * (8 - k // 2)
        t = lax.rem(z + near, 8)
        pltpu.make_async_copy(gb.at[pl.ds(0, 40)], gb.at[pl.ds(0, 40)], r_2.at[t]).wait()
        packed = [gb[pl.ds(t * 64 + p, 8, stride=8), :] for p in range(5)]
        lapse = lap[t]

        def three(f):
            v, r = packed[f // 5], f % 5
            return [roll(v, -6 * r - k) * ups[k - 1] + roll(v, -6 * r + k) * downs[k - 1] for k in (1, 2, 3)]

        for f in range(HALF):
            u1, u2, u3 = three(f)
            v1, v2, v3 = three(f + HALF)
            add(f, t, DAMP[1] * u1 + DAMP[2] * u2 + DAMP[3] * u3)
            add(f + HALF, t,
                DAMP[1] * v1 + DAMP[2] * v2 + DAMP[3] * v3 - 0.5 * lapse * (LAP[1] * u1 + LAP[2] * u2))

    pltpu.make_async_copy(mb.at[pl.ds(0, 315)], mb.at[pl.ds(0, 315)], s_2).wait()


PIECES = 4


def kernel_b(q1, q2, o1, o2, sems):
    copies = []
    for i in range(PIECES):
        part = pl.ds(i * (FIELDS // PIECES), FIELDS // PIECES)
        copies.append(pltpu.make_async_copy(q1.at[part], o1.at[part], sems.at[0, i]))
        copies.append(pltpu.make_async_copy(q2.at[part], o2.at[part], sems.at[1, i]))
    for c in copies:
        c.start()
    for c in copies:
        c.wait()


def local(state, base, accum, owner):
    shape = state.shape
    f32 = jnp.float32
    rows = (FIELDS, 64, LANES)
    hbm = pl.BlockSpec(memory_space=pltpu.HBM)
    vmem = pl.BlockSpec(memory_space=pltpu.VMEM)
    dma = pltpu.SemaphoreType.DMA
    in_hbm = [pltpu.with_memory_space_constraint(v, pltpu.HBM)
              for v in (state.reshape(rows), base.reshape(rows), accum.reshape(rows), owner)]
    q1, q2 = pl.pallas_call(
        kernel_a,
        out_shape=(pltpu.VMEM(rows, f32), pltpu.VMEM(rows, f32)),
        in_specs=[hbm] * 4,
        out_specs=(vmem, vmem),
        scratch_shapes=[
            pltpu.VMEM((FIELDS, 96, LANES), f32),
            pltpu.VMEM(rows, f32),
            pltpu.VMEM((FIELDS, 8, 8, LANES), f32),
            pltpu.VMEM((16, 8, LANES), f32),
            pltpu.VMEM((512, LANES), f32),
            pltpu.VMEM((64, 8, LANES), f32),
            pltpu.VMEM((64, 8, LANES), f32),
            pltpu.VMEM((512, LANES), f32),
            pltpu.VMEM((2, 12, 8, LANES), f32),
            pltpu.VMEM((2, 12, 8, LANES), f32),
            pltpu.VMEM((2, 8, LANES), jnp.int32),
            pltpu.SMEM((2, 8, LANES), jnp.int32),
            pltpu.SMEM((64,), jnp.int32),
            dma((4,)), dma, dma, dma, dma((3,)), dma((3,)), dma, dma, dma, dma((8,)),
        ],
        compiler_params=pltpu.CompilerParams(collective_id=0, has_side_effects=True, vmem_limit_bytes=24 << 20),
    )(*in_hbm)
    o1, o2 = pl.pallas_call(
        kernel_b,
        out_shape=(jax.ShapeDtypeStruct(rows, f32),) * 2,
        in_specs=[vmem, vmem],
        out_specs=(hbm, hbm),
        scratch_shapes=[dma((2, PIECES))],
        compiler_params=pltpu.CompilerParams(vmem_limit_bytes=24 << 20),
    )(q1, q2)
    return o1.reshape(shape), o2.reshape(shape)


def solution(mesh):
    spec = P(None, "gx", ("gy", "gz"), None)
    return jax.shard_map(
        local, mesh=mesh, in_specs=(spec, spec, spec, P()), out_specs=(spec, spec), check_vma=False)
```

```python
import functools

import jax
import jax.numpy as jnp
from jax import lax
from jax.experimental import pallas as pl
from jax.experimental.pallas import tpu as pltpu
from jax.sharding import PartitionSpec as P

MESH = pl.DeviceIdType.MESH
FIELDS, HALF = 24, 12
LANES = 128
C1 = 0.5 * 0.25
C2 = 0.25 / 3.0
DAMP = (-20.0 / 64.0, 15.0 / 64.0, -6.0 / 64.0, 1.0 / 64.0)
LAP = (-30.0 / 12.0, 16.0 / 12.0, -1.0 / 12.0)
ALPHA = LAP[2] / DAMP[3]
BETA = (LAP[1] - LAP[2] * DAMP[2] / DAMP[3]) / DAMP[3]
FAR_FIRST = (4, 3, 5, 2, 6, 1, 7, 0)


def lane_iota(rows=8):
    return lax.broadcasted_iota(jnp.int32, (rows, LANES), 1)


def roll(v, s):
    s %= LANES
    return v if s == 0 else pltpu.roll(v, s, axis=1)


def kernel_a(state, base, accum, owner_hbm, q1, q2,
             xp, sy, rt, lap, mb, rb, fb, gb, xs, xr, tabv, tab, owner,
             s_in, s_tab, s_y, r_y, s_x, r_x, s_1, r_1, s_2, r_2):
    gx, gy, me = lax.axis_index("gx"), lax.axis_index("gy"), lax.axis_index("gz")
    z, w = me // 8, lax.rem(me, 8)

    load_state = pltpu.make_async_copy(state, xp.at[:, pl.ds(16, 64)], s_in.at[0])
    load_base = pltpu.make_async_copy(base, q1, s_in.at[1])
    load_accum = pltpu.make_async_copy(accum, q2, s_in.at[2])
    load_owner = pltpu.make_async_copy(owner_hbm, owner, s_in.at[3])
    load_state.start()
    load_owner.start()

    barrier = pltpu.get_barrier_semaphore()

    def each_peer(action):
        for d in FAR_FIRST:
            @pl.loop(0 if d else 1, 8)
            def _(k):
                action(lax.rem(z + d, 8) * 8 + lax.rem(w + k, 8))

    @each_peer
    def _(peer):
        pl.semaphore_signal(barrier, inc=1, device_id={"gz": peer}, device_id_type=MESH)

    pl.semaphore_signal(barrier, inc=1, device_id={"gy": 1 - gy}, device_id_type=MESH)
    pl.semaphore_signal(barrier, inc=1, device_id={"gx": 1 - gx}, device_id_type=MESH)
    load_base.start()
    load_accum.start()

    load_owner.wait()
    lanes = lane_iota()
    below = jnp.zeros((8, LANES), jnp.int32)
    above = jnp.zeros((8, LANES), jnp.int32)
    for c in range(64):
        hit = lanes == owner[c]
        below = jnp.where(hit, owner[(c + 63) % 64], below)
        above = jnp.where(hit, owner[(c + 1) % 64], above)
    tabv[0] = below
    tabv[1] = above
    load_tab = pltpu.make_async_copy(tabv, tab, s_tab)

    b = lanes % 32
    u = (lanes + 3) % 32
    load_state.wait()
    load_tab.start()

    def row(t):
        return (t // 4) * 32 + t % 4

    def tile(f, t):
        return xp[f, pl.ds(16 + row(t), 8, stride=4), :]

    zero = jnp.zeros((8, LANES), jnp.float32)
    to_high = [jnp.where(b >= 32 - k, DAMP[k], zero) for k in (1, 2, 3)]
    to_low = [jnp.where(b < k, DAMP[k], zero) for k in (1, 2, 3)]

    @pl.loop(0, 8)
    def _(t):
        for p in range(5):
            acc = zero
            for r in range(5 if p < 4 else 4):
                v = tile(p * 5 + r, t)
                x = zero
                for k in (1, 2, 3):
                    x = x + to_high[k - 1] * roll(v, 32 - k) + to_low[k - 1] * roll(v, k - 32)
                window = (u + 32 - 6 * r) % 32 < 6
                acc = jnp.where(window, roll(x, 6 * r), acc)
            mb[pl.ds(t * 64 + p, 8, stride=8), :] = acc

    first = lax.broadcasted_iota(jnp.int32, (8, LANES), 0) < 4
    for f in range(0, FIELDS, 2):
        lo0, lo1 = xp[f, pl.ds(24, 8), :], xp[f + 1, pl.ds(24, 8), :]
        hi0, hi1 = xp[f, pl.ds(64, 8), :], xp[f + 1, pl.ds(64, 8), :]
        xs[0, f // 2] = jnp.where(first, lo0, pltpu.roll(lo1, 4, axis=0))
        xs[1, f // 2] = jnp.where(first, pltpu.roll(hi0, 4, axis=0), hi1)

    pl.semaphore_wait(barrier, 65)

    def five(ref, j):
        if ref.shape[0] == 64:
            return ref.at[j, pl.ds(0, 5)]
        return ref.at[pl.ds(pl.multiple_of(8 * j, 8), 5)]

    def spread(source, target, send, recv):
        @each_peer
        def _(peer):
            pltpu.make_async_remote_copy(
                five(source, peer), five(target, me), send, recv,
                device_id={"gz": peer}, device_id_type=MESH).start()

        pltpu.make_async_copy(five(source, me), five(target, me), recv).start()

    spread(mb, rb, s_1, r_1)

    send_y = pltpu.make_async_remote_copy(
        xp.at[:, pl.ds(16, 64)], sy, s_y, r_y, device_id={"gy": 1 - gy}, device_id_type=MESH)
    send_y.start()
    send_x = [
        pltpu.make_async_remote_copy(
            xp.at[:, pl.ds(16, 8)], xp.at[:, pl.ds(80, 8)], s_x.at[0], r_x.at[0],
            device_id={"gx": 1 - gx}, device_id_type=MESH),
        pltpu.make_async_remote_copy(
            xp.at[:, pl.ds(72, 8)], xp.at[:, pl.ds(8, 8)], s_x.at[1], r_x.at[1],
            device_id={"gx": 1 - gx}, device_id_type=MESH),
        pltpu.make_async_remote_copy(
            xs, xr, s_x.at[2], r_x.at[2], device_id={"gx": 1 - gx}, device_id_type=MESH),
    ]
    for s in send_x:
        s.start()

    load_tab.wait()
    for t in range(8):
        lap[t] = 1.0 + 0.25 * jnp.tanh(tile(0, t))
        total = tile(12, t)
        for f in range(13, 24):
            total = total + tile(f, t)
        lap[8 + t] = lap[t] * (total * (1.0 / 12.0))

    low = [b >= k for k in (1, 2, 3)]
    high = [b < 32 - k for k in (1, 2, 3)]
    left = [lanes >= 32 * k for k in (1, 2, 3)]
    right = [lanes < 128 - 32 * k for k in (1, 2, 3)]

    def plane(f, xg):
        values = [sy[f, pl.ds(xg * 32 + 3, 8, stride=4), :]]
        values += [tile(f, xg * 4 + q) for q in range(4)]
        values += [sy[f, pl.ds(xg * 32, 8, stride=4), :]]
        turned = [[v] + [roll(v, 32 * j) for j in (1, 2, 3)] for v in values]
        sums = []
        for q in range(4):
            v = values[q + 1]
            three = []
            for k in (1, 2, 3):
                plus = jnp.where(right[k - 1], turned[q + 1][4 - k], turned[q + 2][4 - k])
                minus = jnp.where(left[k - 1], turned[q + 1][k], turned[q][k])
                up = jnp.where(high[k - 1], roll(v, -k), 0.0)
                down = jnp.where(low[k - 1], roll(v, k), 0.0)
                three.append((plus + minus) + (up + down))
            sums.append((v, three))
        return sums

    send_y.wait_recv()

    @pl.loop(0, HALF)
    def _(f):
        for xg in range(2):
            us, vs = plane(f, xg), plane(f + HALF, xg)
            for q in range(4):
                t = xg * 4 + q
                lapse, drag = lap[t], lap[8 + t]
                uv, (u1, u2, u3) = us[q]
                vv, (v1, v2, v3) = vs[q]
                damp_u = (2 * DAMP[0]) * uv + DAMP[1] * u1 + DAMP[2] * u2 + DAMP[3] * u3
                damp_v = (2 * DAMP[0]) * vv + DAMP[1] * v1 + DAMP[2] * v2 + DAMP[3] * v3
                laplace = (2 * LAP[0]) * uv + LAP[1] * u1 + LAP[2] * u2
                rt[f, t] = damp_u - 2.0 * lapse * vv
                rt[f + HALF, t] = damp_v + drag * vv - 0.5 * lapse * laplace

    load_base.wait()
    load_accum.wait()
    pltpu.make_async_copy(rb.at[pl.ds(0, 40)], rb.at[pl.ds(0, 40)], r_1).wait()
    kind = (u < 30) & (lax.rem(u, 6) < 3)

    @pl.loop(0, 64, unroll=8)
    def _(g):
        fb[g] = jnp.where(kind, rb[tab[1, 0, g]], rb[tab[0, 0, g]])

    spread(fb, gb, s_2, r_2.at[z])

    for s in send_x:
        s.wait_recv()
    for f in range(0, FIELDS, 2):
        hi, lo = xr[0, f // 2], xr[1, f // 2]
        xp[f, pl.ds(88, 8), :] = hi
        xp[f + 1, pl.ds(88, 8), :] = pltpu.roll(hi, 4, axis=0)
        xp[f, pl.ds(0, 8), :] = pltpu.roll(lo, 4, axis=0)
        xp[f + 1, pl.ds(0, 8), :] = lo

    def add(f, t, rate):
        rows = pl.ds(row(t), 8, stride=4)
        q1[f, rows, :] = q1[f, rows, :] + C1 * rate
        q2[f, rows, :] = q2[f, rows, :] + C2 * rate

    @pl.loop(0, HALF)
    def _(f):
        for t in range(8):
            def shifted(field, k):
                return xp[field, pl.ds(16 + row(t) + 4 * k, 8, stride=4), :]

            def three(field):
                return [shifted(field, k) + shifted(field, -k) for k in (1, 2, 3)]

            uv, vv = shifted(f, 0), shifted(f + HALF, 0)
            u1, u2, u3 = three(f)
            v1, v2, v3 = three(f + HALF)
            damp_u = DAMP[0] * uv + DAMP[1] * u1 + DAMP[2] * u2 + DAMP[3] * u3
            damp_v = DAMP[0] * vv + DAMP[1] * v1 + DAMP[2] * v2 + DAMP[3] * v3
            laplace = LAP[0] * uv + LAP[1] * u1 + LAP[2] * u2
            add(f, t, rt[f, t] + damp_u)
            add(f + HALF, t, rt[f + HALF, t] + damp_v - 0.5 * lap[t] * laplace)

    send_y.wait_send()
    for s in send_x:
        s.wait_send()
    everything = pltpu.make_async_copy(mb.at[pl.ds(0, 315)], mb.at[pl.ds(0, 315)], s_1)
    everything.wait()

    slot = lax.rem(u, 6)
    edge = (b < 3) | (b >= 29)
    edge_1, edge_2 = jnp.where(edge, C1, zero), jnp.where(edge, C2, zero)
    next_up = jnp.where((slot == 3) | (slot == 4), ALPHA, zero)
    next_down = jnp.where((slot == 1) | (slot == 2), ALPHA, zero)
    second_up = jnp.where(slot == 3, BETA, zero)
    second_down = jnp.where(slot == 2, BETA, zero)

    @pl.loop(0, 8)
    def _(k):
        near = lax.rem(k, 2) * ((k + 1) // 2) + (1 - lax.rem(k, 2)) * (8 - k // 2)
        t = lax.rem(z + near, 8)
        pltpu.make_async_copy(gb.at[pl.ds(0, 40)], gb.at[pl.ds(0, 40)], r_2.at[t]).wait()
        packed = [gb[pl.ds(t * 64 + p, 8, stride=8), :] for p in range(5)]
        half_lapse = -0.5 * lap[t]
        laplaces = [
            roll(v, -1) * next_up + roll(v, 1) * next_down + roll(v, -2) * second_up + roll(v, 2) * second_down
            for v in packed[:3]
        ]
        rows = pl.ds(row(t), 8, stride=4)

        def add_edge(f, rate):
            q1[f, rows, :] = q1[f, rows, :] + edge_1 * rate
            q2[f, rows, :] = q2[f, rows, :] + edge_2 * rate

        for f in range(HALF):
            g = f + HALF
            add_edge(f, roll(packed[f // 5], -6 * (f % 5)))
            add_edge(g, roll(packed[g // 5], -6 * (g % 5)) + half_lapse * roll(laplaces[f // 5], -6 * (f % 5)))

    pltpu.make_async_copy(mb.at[pl.ds(0, 315)], mb.at[pl.ds(0, 315)], s_2).wait()


PIECES = 4


def kernel_b(q1, q2, o1, o2, sems):
    copies = []
    for i in range(PIECES):
        part = pl.ds(i * (FIELDS // PIECES), FIELDS // PIECES)
        copies.append(pltpu.make_async_copy(q1.at[part], o1.at[part], sems.at[0, i]))
        copies.append(pltpu.make_async_copy(q2.at[part], o2.at[part], sems.at[1, i]))
    for c in copies:
        c.start()
    for c in copies:
        c.wait()


def local(state, base, accum, owner):
    shape = state.shape
    f32 = jnp.float32
    rows = (FIELDS, 64, LANES)
    hbm = pl.BlockSpec(memory_space=pltpu.HBM)
    vmem = pl.BlockSpec(memory_space=pltpu.VMEM)
    dma = pltpu.SemaphoreType.DMA
    in_hbm = [pltpu.with_memory_space_constraint(v, pltpu.HBM)
              for v in (state.reshape(rows), base.reshape(rows), accum.reshape(rows), owner)]
    q1, q2 = pl.pallas_call(
        kernel_a,
        out_shape=(pltpu.VMEM(rows, f32), pltpu.VMEM(rows, f32)),
        in_specs=[hbm] * 4,
        out_specs=(vmem, vmem),
        scratch_shapes=[
            pltpu.VMEM((FIELDS, 96, LANES), f32),
            pltpu.VMEM(rows, f32),
            pltpu.VMEM((FIELDS, 8, 8, LANES), f32),
            pltpu.VMEM((16, 8, LANES), f32),
            pltpu.VMEM((512, LANES), f32),
            pltpu.VMEM((64, 8, LANES), f32),
            pltpu.VMEM((64, 8, LANES), f32),
            pltpu.VMEM((512, LANES), f32),
            pltpu.VMEM((2, 12, 8, LANES), f32),
            pltpu.VMEM((2, 12, 8, LANES), f32),
            pltpu.VMEM((2, 8, LANES), jnp.int32),
            pltpu.SMEM((2, 8, LANES), jnp.int32),
            pltpu.SMEM((64,), jnp.int32),
            dma((4,)), dma, dma, dma, dma((3,)), dma((3,)), dma, dma, dma, dma((8,)),
        ],
        compiler_params=pltpu.CompilerParams(collective_id=0, has_side_effects=True, vmem_limit_bytes=24 << 20),
    )(*in_hbm)
    o1, o2 = pl.pallas_call(
        kernel_b,
        out_shape=(jax.ShapeDtypeStruct(rows, f32),) * 2,
        in_specs=[vmem, vmem],
        out_specs=(hbm, hbm),
        scratch_shapes=[dma((2, PIECES))],
        compiler_params=pltpu.CompilerParams(vmem_limit_bytes=24 << 20),
    )(q1, q2)
    return o1.reshape(shape), o2.reshape(shape)


def solution(mesh):
    spec = P(None, "gx", ("gy", "gz"), None)
    return jax.shard_map(
        local, mesh=mesh, in_specs=(spec, spec, spec, P()), out_specs=(spec, spec), check_vma=False)
```

```python
import functools

import jax
import jax.numpy as jnp
from jax import lax
from jax.experimental import pallas as pl
from jax.experimental.pallas import tpu as pltpu
from jax.sharding import PartitionSpec as P

MESH = pl.DeviceIdType.MESH
FIELDS, HALF = 24, 12
LANES = 128
C1 = 0.5 * 0.25
C2 = 0.25 / 3.0
DAMP = (-20.0 / 64.0, 15.0 / 64.0, -6.0 / 64.0, 1.0 / 64.0)
LAP = (-30.0 / 12.0, 16.0 / 12.0, -1.0 / 12.0)
ALPHA = LAP[2] / DAMP[3]
BETA = (LAP[1] - LAP[2] * DAMP[2] / DAMP[3]) / DAMP[3]
P2_ORDER = (0, 1, 2, 3, 4, 7, 5, 6)
REACH = 3


def hops(dz, dy, dx):
    return min(dz, 8 - dz) + min(dy, 4 - dy) + dx


NEAR = sorted(
    ((dz, dy, dx) for dz in range(8) for dy in range(4) for dx in range(2) if hops(dz, dy, dx) <= REACH),
    key=lambda d: -hops(*d))


def lane_iota(rows=8):
    return lax.broadcasted_iota(jnp.int32, (rows, LANES), 1)


def roll(v, s):
    s %= LANES
    return v if s == 0 else pltpu.roll(v, s, axis=1)


def kernel_a(state, base, accum, owner_hbm, q1, q2,
             xp, sy, rt, lap, mb, rb, fb, gb, xs, xr, tabv, tab, owner,
             s_in, s_tab, s_y, r_y, s_x, r_x, s_1, r_1, s_2, r_2, beside, beyond):
    gx, gy, me = lax.axis_index("gx"), lax.axis_index("gy"), lax.axis_index("gz")
    z, w = me // 8, lax.rem(me, 8)
    y, x = w // 2, lax.rem(w, 2)

    load_state = pltpu.make_async_copy(state, xp.at[:, pl.ds(16, 64)], s_in.at[0])
    load_base = pltpu.make_async_copy(base, q1, s_in.at[1])
    load_accum = pltpu.make_async_copy(accum, q2, s_in.at[2])
    load_owner = pltpu.make_async_copy(owner_hbm, owner, s_in.at[3])
    load_state.start()
    load_owner.start()

    barrier = pltpu.get_barrier_semaphore()

    def device(dz, dy, dx):
        return (z + dz) % 8 * 8 + (y + dy) % 4 * 2 + (x + dx) % 2

    def pair_of(peer):
        pz, py, px = peer // 8, peer % 8 // 2, peer % 2
        half = pz // 4
        return pz % 4 * 8 + (py + 2 * half) % 4 * 2 + (px + half) % 2

    for d in NEAR[:-1]:
        pl.semaphore_signal(barrier, inc=1, device_id={"gz": device(*d)}, device_id_type=MESH)
    pl.semaphore_signal(barrier, inc=1, device_id={"gy": 1 - gy}, device_id_type=MESH)
    pl.semaphore_signal(barrier, inc=1, device_id={"gx": 1 - gx}, device_id_type=MESH)
    load_base.start()
    load_accum.start()

    load_owner.wait()
    lanes = lane_iota()
    below = jnp.zeros((8, LANES), jnp.int32)
    above = jnp.zeros((8, LANES), jnp.int32)
    for c in range(64):
        hit = lanes == owner[c]
        below = jnp.where(hit, owner[(c + 63) % 64], below)
        above = jnp.where(hit, owner[(c + 1) % 64], above)
    tabv[0] = below
    tabv[1] = above
    load_tab = pltpu.make_async_copy(tabv, tab, s_tab)

    b = lanes % 32
    u = (lanes + 3) % 32
    load_state.wait()
    load_tab.start()

    def row(t):
        return (t // 4) * 32 + t % 4

    def tile(f, t):
        return xp[f, pl.ds(16 + row(t), 8, stride=4), :]

    zero = jnp.zeros((8, LANES), jnp.float32)
    slot = lax.rem(u, 6)
    to_high = [jnp.where((slot < 3) & (slot >= 3 - k), DAMP[k], zero) for k in (1, 2, 3)]
    to_low = [jnp.where((slot >= 3) & (slot < 3 + k), DAMP[k], zero) for k in (1, 2, 3)]
    windows = [(u + 32 - 6 * r) % 32 < 6 for r in range(5)]

    @pl.loop(0, 8)
    def _(t):
        for p in range(5):
            faces = zero
            for r in range(5 if p < 4 else 4):
                faces = jnp.where(windows[r], roll(tile(p * 5 + r, t), 6 * r), faces)
            terms = [roll(faces, 32 - k) * to_high[k - 1] + roll(faces, k - 32) * to_low[k - 1] for k in (1, 2, 3)]
            mb[pl.ds(t % 4 * 128 + t // 4 * 5 + p, 8, stride=16), :] = terms[0] + terms[1] + terms[2]

    pl.semaphore_wait(barrier, 33)

    def pair_rows(ref, j):
        return ref.at[pl.ds(pl.multiple_of(16 * j, 8), 10)]

    for d in NEAR[:-1]:
        peer = device(*d)
        pltpu.make_async_remote_copy(
            pair_rows(mb, pair_of(peer)), rb.at[me, pl.ds(0, 10)], s_1, r_1,
            device_id={"gz": peer}, device_id_type=MESH).start()
    pltpu.make_async_copy(pair_rows(mb, pair_of(me)), rb.at[me, pl.ds(0, 10)], r_1).start()
    pl.semaphore_signal(beside, inc=1, device_id={"gz": device(0, 0, 1)}, device_id_type=MESH)

    first = lax.broadcasted_iota(jnp.int32, (8, LANES), 0) < 4
    for f in range(0, FIELDS, 2):
        lo0, lo1 = xp[f, pl.ds(24, 8), :], xp[f + 1, pl.ds(24, 8), :]
        hi0, hi1 = xp[f, pl.ds(64, 8), :], xp[f + 1, pl.ds(64, 8), :]
        xs[0, f // 2] = jnp.where(first, lo0, pltpu.roll(lo1, 4, axis=0))
        xs[1, f // 2] = jnp.where(first, pltpu.roll(hi0, 4, axis=0), hi1)

    send_y = pltpu.make_async_remote_copy(
        xp.at[:, pl.ds(16, 64)], sy, s_y, r_y, device_id={"gy": 1 - gy}, device_id_type=MESH)
    send_y.start()
    send_x = [
        pltpu.make_async_remote_copy(
            xp.at[:, pl.ds(16, 8)], xp.at[:, pl.ds(80, 8)], s_x.at[0], r_x.at[0],
            device_id={"gx": 1 - gx}, device_id_type=MESH),
        pltpu.make_async_remote_copy(
            xp.at[:, pl.ds(72, 8)], xp.at[:, pl.ds(8, 8)], s_x.at[1], r_x.at[1],
            device_id={"gx": 1 - gx}, device_id_type=MESH),
        pltpu.make_async_remote_copy(
            xs, xr, s_x.at[2], r_x.at[2], device_id={"gx": 1 - gx}, device_id_type=MESH),
    ]
    for s in send_x:
        s.start()

    pl.semaphore_wait(beside, 1)
    pl.semaphore_signal(beyond, inc=1, device_id={"gz": device(6, 3, 0)}, device_id_type=MESH)

    load_tab.wait()
    for t in range(8):
        lap[t] = 1.0 + 0.25 * jnp.tanh(tile(0, t))
        total = tile(12, t)
        for f in range(13, 24):
            total = total + tile(f, t)
        lap[8 + t] = lap[t] * (total * (1.0 / 12.0))

    low = [b >= k for k in (1, 2, 3)]
    high = [b < 32 - k for k in (1, 2, 3)]
    left = [lanes >= 32 * k for k in (1, 2, 3)]
    right = [lanes < 128 - 32 * k for k in (1, 2, 3)]

    def plane(f, xg):
        values = [sy[f, pl.ds(xg * 32 + 3, 8, stride=4), :]]
        values += [tile(f, xg * 4 + q) for q in range(4)]
        values += [sy[f, pl.ds(xg * 32, 8, stride=4), :]]
        turned = [[v] + [roll(v, 32 * j) for j in (1, 2, 3)] for v in values]
        sums = []
        for q in range(4):
            v = values[q + 1]
            three = []
            for k in (1, 2, 3):
                plus = jnp.where(right[k - 1], turned[q + 1][4 - k], turned[q + 2][4 - k])
                minus = jnp.where(left[k - 1], turned[q + 1][k], turned[q][k])
                up = jnp.where(high[k - 1], roll(v, -k), 0.0)
                down = jnp.where(low[k - 1], roll(v, k), 0.0)
                three.append((plus + minus) + (up + down))
            sums.append((v, three))
        return sums

    send_y.wait_recv()

    @pl.loop(0, HALF)
    def _(f):
        for xg in range(2):
            us, vs = plane(f, xg), plane(f + HALF, xg)
            for q in range(4):
                t = xg * 4 + q
                lapse, drag = lap[t], lap[8 + t]
                uv, (u1, u2, u3) = us[q]
                vv, (v1, v2, v3) = vs[q]
                damp_u = (2 * DAMP[0]) * uv + DAMP[1] * u1 + DAMP[2] * u2 + DAMP[3] * u3
                damp_v = (2 * DAMP[0]) * vv + DAMP[1] * v1 + DAMP[2] * v2 + DAMP[3] * v3
                laplace = (2 * LAP[0]) * uv + LAP[1] * u1 + LAP[2] * u2
                rt[f, t] = damp_u - 2.0 * lapse * vv
                rt[f + HALF, t] = damp_v + drag * vv - 0.5 * lapse * laplace

    load_base.wait()
    load_accum.wait()
    pltpu.make_async_copy(rb.at[pl.ds(0, 20)], rb.at[pl.ds(0, 20)], r_1).wait()
    pl.semaphore_wait(beyond, 1)
    kind = slot < 3
    my_slot = z // 4 * 32 + pair_of(me)

    def permute(plane):
        for k in range(8):
            g = plane * 8 + k
            below_g, above_g = rb[tab[0, 0, g]], rb[tab[1, 0, g]]
            fb[g] = jnp.concatenate(
                [jnp.where(kind, above_g[h:h + 8], below_g[h:h + 8]) for h in (0, 8)], axis=0)

    permute(P2_ORDER[0])
    for n, plane in enumerate(P2_ORDER):
        if n < 7:
            permute(P2_ORDER[n + 1])

        @pl.loop(0, 8)
        def _(k):
            peer = plane * 8 + k

            @pl.when(peer != me)
            def _():
                pltpu.make_async_remote_copy(
                    fb.at[peer, pl.ds(0, 10)], pair_rows(gb, my_slot), s_2, r_2.at[z],
                    device_id={"gz": peer}, device_id_type=MESH).start()

    pltpu.make_async_copy(fb.at[me, pl.ds(0, 10)], pair_rows(gb, my_slot), r_2.at[z]).start()

    for s in send_x:
        s.wait_recv()
    for f in range(0, FIELDS, 2):
        hi, lo = xr[0, f // 2], xr[1, f // 2]
        xp[f, pl.ds(88, 8), :] = hi
        xp[f + 1, pl.ds(88, 8), :] = pltpu.roll(hi, 4, axis=0)
        xp[f, pl.ds(0, 8), :] = pltpu.roll(lo, 4, axis=0)
        xp[f + 1, pl.ds(0, 8), :] = lo

    def add(f, t, rate):
        rows = pl.ds(row(t), 8, stride=4)
        q1[f, rows, :] = q1[f, rows, :] + C1 * rate
        q2[f, rows, :] = q2[f, rows, :] + C2 * rate

    @pl.loop(0, HALF)
    def _(f):
        for t in range(8):
            def shifted(field, k):
                return xp[field, pl.ds(16 + row(t) + 4 * k, 8, stride=4), :]

            def three(field):
                return [shifted(field, k) + shifted(field, -k) for k in (1, 2, 3)]

            uv, vv = shifted(f, 0), shifted(f + HALF, 0)
            u1, u2, u3 = three(f)
            v1, v2, v3 = three(f + HALF)
            damp_u = DAMP[0] * uv + DAMP[1] * u1 + DAMP[2] * u2 + DAMP[3] * u3
            damp_v = DAMP[0] * vv + DAMP[1] * v1 + DAMP[2] * v2 + DAMP[3] * v3
            laplace = LAP[0] * uv + LAP[1] * u1 + LAP[2] * u2
            add(f, t, rt[f, t] + damp_u)
            add(f + HALF, t, rt[f + HALF, t] + damp_v - 0.5 * lap[t] * laplace)

    send_y.wait_send()
    for s in send_x:
        s.wait_send()
    pltpu.make_async_copy(mb.at[pl.ds(0, 310)], mb.at[pl.ds(0, 310)], s_1).wait()

    edge = (b < 3) | (b >= 29)
    edge_1, edge_2 = jnp.where(edge, C1, zero), jnp.where(edge, C2, zero)
    next_up = jnp.where((slot == 3) | (slot == 4), ALPHA, zero)
    next_down = jnp.where((slot == 1) | (slot == 2), ALPHA, zero)
    second_up = jnp.where(slot == 3, BETA, zero)
    second_down = jnp.where(slot == 2, BETA, zero)

    sub = lax.broadcasted_iota(jnp.int32, (8, LANES), 0)

    def reached(neighbour, t):
        nz, ny, nx = neighbour // 8, neighbour % 8 // 2, neighbour % 2
        dz, dy = jnp.abs(nz - t), jnp.abs(sub // 2 - ny)
        dx = jnp.abs(sub % 2 - nx)
        return jnp.minimum(dz, 8 - dz) + jnp.minimum(dy, 4 - dy) + dx

    chosen = []
    for t in range(4):
        chosen.append(jnp.where(kind, reached(tab[1, 0, me], t), reached(tab[0, 0, me], t)) <= REACH)

    for t in (1, 5, 0, 4, 2, 6, 3, 7):
        if t < 4:
            for plane in (t, t + 4):
                pltpu.make_async_copy(gb.at[pl.ds(0, 80)], gb.at[pl.ds(0, 80)], r_2.at[plane]).wait()
        packed = []
        for p in range(5):
            start = t % 4 * 128 + t // 4 * 5 + p
            packed.append(jnp.where(
                chosen[t % 4],
                gb[pl.ds(start, 8, stride=16), :],
                gb[pl.ds(512 + start, 8, stride=16), :]))
        half_lapse = -0.5 * lap[t]
        laplaces = [
            roll(v, -1) * next_up + roll(v, 1) * next_down + roll(v, -2) * second_up + roll(v, 2) * second_down
            for v in packed[:3]
        ]
        rows = pl.ds(row(t), 8, stride=4)

        def add_edge(f, rate):
            q1[f, rows, :] = q1[f, rows, :] + edge_1 * rate
            q2[f, rows, :] = q2[f, rows, :] + edge_2 * rate

        for f in range(HALF):
            g = f + HALF
            add_edge(f, roll(packed[f // 5], -6 * (f % 5)))
            add_edge(g, roll(packed[g // 5], -6 * (g % 5)) + half_lapse * roll(laplaces[f // 5], -6 * (f % 5)))

    pltpu.make_async_copy(gb.at[pl.ds(0, 630)], gb.at[pl.ds(0, 630)], s_2).wait()


PIECES = 1


def kernel_b(q1, q2, o1, o2, sems):
    copies = []
    for i in range(PIECES):
        part = pl.ds(i * (FIELDS // PIECES), FIELDS // PIECES)
        copies.append(pltpu.make_async_copy(q1.at[part], o1.at[part], sems.at[0, i]))
        copies.append(pltpu.make_async_copy(q2.at[part], o2.at[part], sems.at[1, i]))
    for c in copies:
        c.start()
    for c in copies:
        c.wait()


def local(state, base, accum, owner):
    shape = state.shape
    f32 = jnp.float32
    rows = (FIELDS, 64, LANES)
    hbm = pl.BlockSpec(memory_space=pltpu.HBM)
    vmem = pl.BlockSpec(memory_space=pltpu.VMEM)
    dma = pltpu.SemaphoreType.DMA
    in_hbm = [pltpu.with_memory_space_constraint(v, pltpu.HBM)
              for v in (state.reshape(rows), base.reshape(rows), accum.reshape(rows), owner)]
    q1, q2 = pl.pallas_call(
        kernel_a,
        out_shape=(pltpu.VMEM(rows, f32), pltpu.VMEM(rows, f32)),
        in_specs=[hbm] * 4,
        out_specs=(vmem, vmem),
        scratch_shapes=[
            pltpu.VMEM((FIELDS, 96, LANES), f32),
            pltpu.VMEM(rows, f32),
            pltpu.VMEM((FIELDS, 8, 8, LANES), f32),
            pltpu.VMEM((16, 8, LANES), f32),
            pltpu.VMEM((512, LANES), f32),
            pltpu.VMEM((64, 16, LANES), f32),
            pltpu.VMEM((64, 16, LANES), f32),
            pltpu.VMEM((1024, LANES), f32),
            pltpu.VMEM((2, 12, 8, LANES), f32),
            pltpu.VMEM((2, 12, 8, LANES), f32),
            pltpu.VMEM((2, 8, LANES), jnp.int32),
            pltpu.SMEM((2, 8, LANES), jnp.int32),
            pltpu.SMEM((64,), jnp.int32),
            dma((4,)), dma, dma, dma, dma((3,)), dma((3,)), dma, dma, dma, dma((8,)),
            pltpu.SemaphoreType.REGULAR, pltpu.SemaphoreType.REGULAR,
        ],
        compiler_params=pltpu.CompilerParams(collective_id=0, has_side_effects=True, vmem_limit_bytes=24 << 20),
    )(*in_hbm)
    o1, o2 = pl.pallas_call(
        kernel_b,
        out_shape=(jax.ShapeDtypeStruct(rows, f32),) * 2,
        in_specs=[vmem, vmem],
        out_specs=(hbm, hbm),
        scratch_shapes=[dma((2, PIECES))],
        compiler_params=pltpu.CompilerParams(vmem_limit_bytes=24 << 20),
    )(q1, q2)
    return o1.reshape(shape), o2.reshape(shape)


def solution(mesh):
    spec = P(None, "gx", ("gy", "gz"), None)
    return jax.shard_map(
        local, mesh=mesh, in_specs=(spec, spec, spec, P()), out_specs=(spec, spec), check_vma=False)
```

```python
import functools

import jax
import jax.numpy as jnp
from jax import lax
from jax.experimental import pallas as pl
from jax.experimental.pallas import tpu as pltpu
from jax.sharding import PartitionSpec as P

MESH = pl.DeviceIdType.MESH
FIELDS, HALF = 24, 12
LANES = 128
C1 = 0.5 * 0.25
C2 = 0.25 / 3.0
DAMP = (-20.0 / 64.0, 15.0 / 64.0, -6.0 / 64.0, 1.0 / 64.0)
LAP = (-30.0 / 12.0, 16.0 / 12.0, -1.0 / 12.0)
ALPHA = LAP[2] / DAMP[3]
BETA = (LAP[1] - LAP[2] * DAMP[2] / DAMP[3]) / DAMP[3]
P2_ORDER = (0, 1, 2, 3, 4, 7, 5, 6)
REACH = 3


def hops(dz, dy, dx):
    return min(dz, 8 - dz) + min(dy, 4 - dy) + dx


NEAR = sorted(
    ((dz, dy, dx) for dz in range(8) for dy in range(4) for dx in range(2) if hops(dz, dy, dx) <= REACH),
    key=lambda d: -hops(*d))


def lane_iota(rows=8):
    return lax.broadcasted_iota(jnp.int32, (rows, LANES), 1)


def roll(v, s):
    s %= LANES
    return v if s == 0 else pltpu.roll(v, s, axis=1)


def kernel_a(state, base, accum, owner_hbm, q1, q2,
             xp, sy, rt, lap, mb, rb, fb, gb, xs, xr, tabv, tab, owner,
             s_in, s_tab, s_y, r_y, s_x, r_x, s_1, r_1, s_2, r_2, beside, beyond):
    gx, gy, me = lax.axis_index("gx"), lax.axis_index("gy"), lax.axis_index("gz")
    z, w = me // 8, lax.rem(me, 8)
    y, x = w // 2, lax.rem(w, 2)

    load_state = pltpu.make_async_copy(state, xp.at[:, pl.ds(16, 64)], s_in.at[0])
    load_base = pltpu.make_async_copy(base, q1, s_in.at[1])
    load_accum = pltpu.make_async_copy(accum, q2, s_in.at[2])
    load_owner = pltpu.make_async_copy(owner_hbm, owner, s_in.at[3])
    load_state.start()
    load_owner.start()

    barrier = pltpu.get_barrier_semaphore()

    zs = [lax.rem(z + d, 8) for d in range(8)]
    ws = [[lax.rem(y + dy, 4) * 2 + lax.rem(x + dx, 2) for dx in range(2)] for dy in range(4)]
    halves = [v // 4 for v in zs[:4]]
    halves += [1 - v for v in halves]
    planes = [lax.rem(z + d, 4) * 8 for d in range(4)]

    def device(dz, dy, dx):
        return zs[dz] * 8 + ws[dy][dx]

    def pair_at(dz, dy, dx):
        across = ws[(dy + 2) % 4][1 - dx] - ws[dy][dx]
        return planes[dz % 4] + ws[dy][dx] + halves[dz] * across

    for d in NEAR[:-1]:
        pl.semaphore_signal(barrier, inc=1, device_id={"gz": device(*d)}, device_id_type=MESH)
    pl.semaphore_signal(barrier, inc=1, device_id={"gy": 1 - gy}, device_id_type=MESH)
    pl.semaphore_signal(barrier, inc=1, device_id={"gx": 1 - gx}, device_id_type=MESH)
    load_base.start()
    load_accum.start()

    load_owner.wait()
    lanes = lane_iota()
    below = jnp.zeros((8, LANES), jnp.int32)
    above = jnp.zeros((8, LANES), jnp.int32)
    for c in range(64):
        hit = lanes == owner[c]
        below = jnp.where(hit, owner[(c + 63) % 64], below)
        above = jnp.where(hit, owner[(c + 1) % 64], above)
    tabv[0] = below
    tabv[1] = above
    load_tab = pltpu.make_async_copy(tabv, tab, s_tab)

    b = lanes % 32
    u = (lanes + 3) % 32
    load_state.wait()
    load_tab.start()

    def row(t):
        return (t // 4) * 32 + t % 4

    def tile(f, t):
        return xp[f, pl.ds(16 + row(t), 8, stride=4), :]

    zero = jnp.zeros((8, LANES), jnp.float32)
    slot = lax.rem(u, 6)
    to_high = [jnp.where((slot < 3) & (slot >= 3 - k), DAMP[k], zero) for k in (1, 2, 3)]
    to_low = [jnp.where((slot >= 3) & (slot < 3 + k), DAMP[k], zero) for k in (1, 2, 3)]
    windows = [(u + 32 - 6 * r) % 32 < 6 for r in range(5)]

    @pl.loop(0, 8)
    def _(t):
        for p in range(5):
            faces = zero
            for r in range(5 if p < 4 else 4):
                faces = jnp.where(windows[r], roll(tile(p * 5 + r, t), 6 * r), faces)
            terms = [roll(faces, 32 - k) * to_high[k - 1] + roll(faces, k - 32) * to_low[k - 1] for k in (1, 2, 3)]
            mb[pl.ds(t % 4 * 128 + t // 4 * 5 + p, 8, stride=16), :] = terms[0] + terms[1] + terms[2]

    pl.semaphore_wait(barrier, 33)

    def pair_rows(ref, j):
        return ref.at[pl.ds(pl.multiple_of(16 * j, 8), 10)]

    for d in NEAR[:-1]:
        peer = device(*d)
        pltpu.make_async_remote_copy(
            pair_rows(mb, pair_at(*d)), rb.at[me, pl.ds(0, 10)], s_1, r_1,
            device_id={"gz": peer}, device_id_type=MESH).start()
    my_pair = pair_at(0, 0, 0)
    pltpu.make_async_copy(pair_rows(mb, my_pair), rb.at[me, pl.ds(0, 10)], r_1).start()
    pl.semaphore_signal(beside, inc=1, device_id={"gz": device(0, 0, 1)}, device_id_type=MESH)

    first = lax.broadcasted_iota(jnp.int32, (8, LANES), 0) < 4
    for f in range(0, FIELDS, 2):
        lo0, lo1 = xp[f, pl.ds(24, 8), :], xp[f + 1, pl.ds(24, 8), :]
        hi0, hi1 = xp[f, pl.ds(64, 8), :], xp[f + 1, pl.ds(64, 8), :]
        xs[0, f // 2] = jnp.where(first, lo0, pltpu.roll(lo1, 4, axis=0))
        xs[1, f // 2] = jnp.where(first, pltpu.roll(hi0, 4, axis=0), hi1)

    send_y = pltpu.make_async_remote_copy(
        xp.at[:, pl.ds(16, 64)], sy, s_y, r_y, device_id={"gy": 1 - gy}, device_id_type=MESH)
    send_y.start()
    send_x = [
        pltpu.make_async_remote_copy(
            xp.at[:, pl.ds(16, 8)], xp.at[:, pl.ds(80, 8)], s_x.at[0], r_x.at[0],
            device_id={"gx": 1 - gx}, device_id_type=MESH),
        pltpu.make_async_remote_copy(
            xp.at[:, pl.ds(72, 8)], xp.at[:, pl.ds(8, 8)], s_x.at[1], r_x.at[1],
            device_id={"gx": 1 - gx}, device_id_type=MESH),
        pltpu.make_async_remote_copy(
            xs, xr, s_x.at[2], r_x.at[2], device_id={"gx": 1 - gx}, device_id_type=MESH),
    ]
    for s in send_x:
        s.start()

    pl.semaphore_wait(beside, 1)
    pl.semaphore_signal(beyond, inc=1, device_id={"gz": device(6, 3, 0)}, device_id_type=MESH)

    load_tab.wait()
    for t in range(8):
        lap[t] = 1.0 + 0.25 * jnp.tanh(tile(0, t))
        total = tile(12, t)
        for f in range(13, 24):
            total = total + tile(f, t)
        lap[8 + t] = lap[t] * (total * (1.0 / 12.0))

    low = [b >= k for k in (1, 2, 3)]
    high = [b < 32 - k for k in (1, 2, 3)]
    left = [lanes >= 32 * k for k in (1, 2, 3)]
    right = [lanes < 128 - 32 * k for k in (1, 2, 3)]

    def plane(f, xg):
        values = [sy[f, pl.ds(xg * 32 + 3, 8, stride=4), :]]
        values += [tile(f, xg * 4 + q) for q in range(4)]
        values += [sy[f, pl.ds(xg * 32, 8, stride=4), :]]
        turned = [[v] + [roll(v, 32 * j) for j in (1, 2, 3)] for v in values]
        sums = []
        for q in range(4):
            v = values[q + 1]
            three = []
            for k in (1, 2, 3):
                plus = jnp.where(right[k - 1], turned[q + 1][4 - k], turned[q + 2][4 - k])
                minus = jnp.where(left[k - 1], turned[q + 1][k], turned[q][k])
                up = jnp.where(high[k - 1], roll(v, -k), 0.0)
                down = jnp.where(low[k - 1], roll(v, k), 0.0)
                three.append((plus + minus) + (up + down))
            sums.append((v, three))
        return sums

    send_y.wait_recv()

    @pl.loop(0, HALF)
    def _(f):
        for xg in range(2):
            us, vs = plane(f, xg), plane(f + HALF, xg)
            for q in range(4):
                t = xg * 4 + q
                lapse, drag = lap[t], lap[8 + t]
                uv, (u1, u2, u3) = us[q]
                vv, (v1, v2, v3) = vs[q]
                damp_u = (2 * DAMP[0]) * uv + DAMP[1] * u1 + DAMP[2] * u2 + DAMP[3] * u3
                damp_v = (2 * DAMP[0]) * vv + DAMP[1] * v1 + DAMP[2] * v2 + DAMP[3] * v3
                laplace = (2 * LAP[0]) * uv + LAP[1] * u1 + LAP[2] * u2
                rt[f, t] = damp_u - 2.0 * lapse * vv
                rt[f + HALF, t] = damp_v + drag * vv - 0.5 * lapse * laplace

    load_base.wait()
    load_accum.wait()
    pltpu.make_async_copy(rb.at[pl.ds(0, 20)], rb.at[pl.ds(0, 20)], r_1).wait()
    pl.semaphore_wait(beyond, 1)
    kind = slot < 3
    my_slot = z // 4 * 32 + my_pair

    def permute(plane):
        for k in range(8):
            g = plane * 8 + k
            below_g, above_g = rb[tab[0, 0, g]], rb[tab[1, 0, g]]
            fb[g] = jnp.concatenate(
                [jnp.where(kind, above_g[h:h + 8], below_g[h:h + 8]) for h in (0, 8)], axis=0)

    permute(P2_ORDER[0])
    for n, plane in enumerate(P2_ORDER):
        if n < 7:
            permute(P2_ORDER[n + 1])

        @pl.loop(0, 8)
        def _(k):
            peer = plane * 8 + k

            @pl.when(peer != me)
            def _():
                pltpu.make_async_remote_copy(
                    fb.at[peer, pl.ds(0, 10)], pair_rows(gb, my_slot), s_2, r_2.at[z],
                    device_id={"gz": peer}, device_id_type=MESH).start()

    pltpu.make_async_copy(fb.at[me, pl.ds(0, 10)], pair_rows(gb, my_slot), r_2.at[z]).start()

    for s in send_x:
        s.wait_recv()
    for f in range(0, FIELDS, 2):
        hi, lo = xr[0, f // 2], xr[1, f // 2]
        xp[f, pl.ds(88, 8), :] = hi
        xp[f + 1, pl.ds(88, 8), :] = pltpu.roll(hi, 4, axis=0)
        xp[f, pl.ds(0, 8), :] = pltpu.roll(lo, 4, axis=0)
        xp[f + 1, pl.ds(0, 8), :] = lo

    def add(f, t, rate):
        rows = pl.ds(row(t), 8, stride=4)
        q1[f, rows, :] = q1[f, rows, :] + C1 * rate
        q2[f, rows, :] = q2[f, rows, :] + C2 * rate

    @pl.loop(0, HALF)
    def _(f):
        for t in range(8):
            def shifted(field, k):
                return xp[field, pl.ds(16 + row(t) + 4 * k, 8, stride=4), :]

            def three(field):
                return [shifted(field, k) + shifted(field, -k) for k in (1, 2, 3)]

            uv, vv = shifted(f, 0), shifted(f + HALF, 0)
            u1, u2, u3 = three(f)
            v1, v2, v3 = three(f + HALF)
            damp_u = DAMP[0] * uv + DAMP[1] * u1 + DAMP[2] * u2 + DAMP[3] * u3
            damp_v = DAMP[0] * vv + DAMP[1] * v1 + DAMP[2] * v2 + DAMP[3] * v3
            laplace = LAP[0] * uv + LAP[1] * u1 + LAP[2] * u2
            add(f, t, rt[f, t] + damp_u)
            add(f + HALF, t, rt[f + HALF, t] + damp_v - 0.5 * lap[t] * laplace)

    send_y.wait_send()
    for s in send_x:
        s.wait_send()
    pltpu.make_async_copy(mb.at[pl.ds(0, 310)], mb.at[pl.ds(0, 310)], s_1).wait()

    edge = (b < 3) | (b >= 29)
    edge_1, edge_2 = jnp.where(edge, C1, zero), jnp.where(edge, C2, zero)
    next_up = jnp.where((slot == 3) | (slot == 4), ALPHA, zero)
    next_down = jnp.where((slot == 1) | (slot == 2), ALPHA, zero)
    second_up = jnp.where(slot == 3, BETA, zero)
    second_down = jnp.where(slot == 2, BETA, zero)

    sub = lax.broadcasted_iota(jnp.int32, (8, LANES), 0)

    def reached(neighbour, t):
        nz, ny, nx = neighbour // 8, neighbour % 8 // 2, neighbour % 2
        dz, dy = jnp.abs(nz - t), jnp.abs(sub // 2 - ny)
        dx = jnp.abs(sub % 2 - nx)
        return jnp.minimum(dz, 8 - dz) + jnp.minimum(dy, 4 - dy) + dx

    chosen = []
    for t in range(4):
        chosen.append(jnp.where(kind, reached(tab[1, 0, me], t), reached(tab[0, 0, me], t)) <= REACH)

    for t in (1, 5, 0, 4, 2, 6, 3, 7):
        if t < 4:
            for plane in (t, t + 4):
                pltpu.make_async_copy(gb.at[pl.ds(0, 80)], gb.at[pl.ds(0, 80)], r_2.at[plane]).wait()
        packed = []
        for p in range(5):
            start = t % 4 * 128 + t // 4 * 5 + p
            packed.append(jnp.where(
                chosen[t % 4],
                gb[pl.ds(start, 8, stride=16), :],
                gb[pl.ds(512 + start, 8, stride=16), :]))
        half_lapse = -0.5 * lap[t]
        laplaces = [
            roll(v, -1) * next_up + roll(v, 1) * next_down + roll(v, -2) * second_up + roll(v, 2) * second_down
            for v in packed[:3]
        ]
        rows = pl.ds(row(t), 8, stride=4)

        def add_edge(f, rate):
            q1[f, rows, :] = q1[f, rows, :] + edge_1 * rate
            q2[f, rows, :] = q2[f, rows, :] + edge_2 * rate

        for f in range(HALF):
            g = f + HALF
            add_edge(f, roll(packed[f // 5], -6 * (f % 5)))
            add_edge(g, roll(packed[g // 5], -6 * (g % 5)) + half_lapse * roll(laplaces[f // 5], -6 * (f % 5)))

    pltpu.make_async_copy(gb.at[pl.ds(0, 630)], gb.at[pl.ds(0, 630)], s_2).wait()


PIECES = 1


def kernel_b(q1, q2, o1, o2, sems):
    copies = []
    for i in range(PIECES):
        part = pl.ds(i * (FIELDS // PIECES), FIELDS // PIECES)
        copies.append(pltpu.make_async_copy(q1.at[part], o1.at[part], sems.at[0, i]))
        copies.append(pltpu.make_async_copy(q2.at[part], o2.at[part], sems.at[1, i]))
    for c in copies:
        c.start()
    for c in copies:
        c.wait()


def local(state, base, accum, owner):
    shape = state.shape
    f32 = jnp.float32
    rows = (FIELDS, 64, LANES)
    hbm = pl.BlockSpec(memory_space=pltpu.HBM)
    vmem = pl.BlockSpec(memory_space=pltpu.VMEM)
    dma = pltpu.SemaphoreType.DMA
    in_hbm = [pltpu.with_memory_space_constraint(v, pltpu.HBM)
              for v in (state.reshape(rows), base.reshape(rows), accum.reshape(rows), owner)]
    q1, q2 = pl.pallas_call(
        kernel_a,
        out_shape=(pltpu.VMEM(rows, f32), pltpu.VMEM(rows, f32)),
        in_specs=[hbm] * 4,
        out_specs=(vmem, vmem),
        scratch_shapes=[
            pltpu.VMEM((FIELDS, 96, LANES), f32),
            pltpu.VMEM(rows, f32),
            pltpu.VMEM((FIELDS, 8, 8, LANES), f32),
            pltpu.VMEM((16, 8, LANES), f32),
            pltpu.VMEM((512, LANES), f32),
            pltpu.VMEM((64, 16, LANES), f32),
            pltpu.VMEM((64, 16, LANES), f32),
            pltpu.VMEM((1024, LANES), f32),
            pltpu.VMEM((2, 12, 8, LANES), f32),
            pltpu.VMEM((2, 12, 8, LANES), f32),
            pltpu.VMEM((2, 8, LANES), jnp.int32),
            pltpu.SMEM((2, 8, LANES), jnp.int32),
            pltpu.SMEM((64,), jnp.int32),
            dma((4,)), dma, dma, dma, dma((3,)), dma((3,)), dma, dma, dma, dma((8,)),
            pltpu.SemaphoreType.REGULAR, pltpu.SemaphoreType.REGULAR,
        ],
        compiler_params=pltpu.CompilerParams(collective_id=0, has_side_effects=True, vmem_limit_bytes=24 << 20),
    )(*in_hbm)
    o1, o2 = pl.pallas_call(
        kernel_b,
        out_shape=(jax.ShapeDtypeStruct(rows, f32),) * 2,
        in_specs=[vmem, vmem],
        out_specs=(hbm, hbm),
        scratch_shapes=[dma((2, PIECES))],
        compiler_params=pltpu.CompilerParams(vmem_limit_bytes=24 << 20),
    )(q1, q2)
    return o1.reshape(shape), o2.reshape(shape)


def solution(mesh):
    spec = P(None, "gx", ("gy", "gz"), None)
    return jax.shard_map(
        local, mesh=mesh, in_specs=(spec, spec, spec, P()), out_specs=(spec, spec), check_vma=False)
```

```python
import functools

import jax
import jax.numpy as jnp
from jax import lax
from jax.experimental import pallas as pl
from jax.experimental.pallas import tpu as pltpu
from jax.sharding import PartitionSpec as P

MESH = pl.DeviceIdType.MESH
FIELDS, HALF = 24, 12
LANES = 128
C1 = 0.5 * 0.25
C2 = 0.25 / 3.0
DAMP = (-20.0 / 64.0, 15.0 / 64.0, -6.0 / 64.0, 1.0 / 64.0)
LAP = (-30.0 / 12.0, 16.0 / 12.0, -1.0 / 12.0)
ALPHA = LAP[2] / DAMP[3]
BETA = (LAP[1] - LAP[2] * DAMP[2] / DAMP[3]) / DAMP[3]
REACH = 3


def hops(dz, dy, dx):
    return min(dz, 8 - dz) + min(dy, 4 - dy) + dx


NEAR = sorted(
    ((dz, dy, dx) for dz in range(8) for dy in range(4) for dx in range(2) if hops(dz, dy, dx) <= REACH),
    key=lambda d: -hops(*d))


def lane_iota(rows=8):
    return lax.broadcasted_iota(jnp.int32, (rows, LANES), 1)


def roll(v, s):
    s %= LANES
    return v if s == 0 else pltpu.roll(v, s, axis=1)


def kernel_a(state, base, accum, owner_hbm, q1, q2,
             xp, sy, rt, lap, mb, rb, fb, gb, xs, xr, tabv, tab, owner,
             s_in, s_tab, s_y, r_y, s_x, r_x, s_1, r_1, s_2, r_2, beside, beyond):
    gx, gy, me = lax.axis_index("gx"), lax.axis_index("gy"), lax.axis_index("gz")
    z, w = me // 8, lax.rem(me, 8)
    y, x = w // 2, lax.rem(w, 2)

    load_state = pltpu.make_async_copy(state, xp.at[:, pl.ds(16, 64)], s_in.at[0])
    load_base = pltpu.make_async_copy(base, q1, s_in.at[1])
    load_accum = pltpu.make_async_copy(accum, q2, s_in.at[2])
    load_owner = pltpu.make_async_copy(owner_hbm, owner, s_in.at[3])
    load_state.start()
    load_owner.start()

    barrier = pltpu.get_barrier_semaphore()

    zs = [lax.rem(z + d, 8) for d in range(8)]
    ws = [[lax.rem(y + dy, 4) * 2 + lax.rem(x + dx, 2) for dx in range(2)] for dy in range(4)]
    halves = [v // 4 for v in zs[:4]]
    halves += [1 - v for v in halves]
    planes = [lax.rem(z + d, 4) * 8 for d in range(4)]

    def device(dz, dy, dx):
        return zs[dz] * 8 + ws[dy][dx]

    def pair_at(dz, dy, dx):
        across = ws[(dy + 2) % 4][1 - dx] - ws[dy][dx]
        return planes[dz % 4] + ws[dy][dx] + halves[dz] * across

    for d in NEAR[:-1]:
        pl.semaphore_signal(barrier, inc=1, device_id={"gz": device(*d)}, device_id_type=MESH)
    pl.semaphore_signal(barrier, inc=1, device_id={"gy": 1 - gy}, device_id_type=MESH)
    pl.semaphore_signal(barrier, inc=1, device_id={"gx": 1 - gx}, device_id_type=MESH)
    load_base.start()
    load_accum.start()

    load_owner.wait()
    lanes = lane_iota()
    below = jnp.zeros((8, LANES), jnp.int32)
    above = jnp.zeros((8, LANES), jnp.int32)
    for c in range(64):
        hit = lanes == owner[c]
        below = jnp.where(hit, owner[(c + 63) % 64], below)
        above = jnp.where(hit, owner[(c + 1) % 64], above)
    tabv[0] = below
    tabv[1] = above
    load_tab = pltpu.make_async_copy(tabv, tab, s_tab)

    b = lanes % 32
    u = (lanes + 3) % 32
    load_state.wait()
    load_tab.start()

    def row(t):
        return (t // 4) * 32 + t % 4

    def tile(f, t):
        return xp[f, pl.ds(16 + row(t), 8, stride=4), :]

    zero = jnp.zeros((8, LANES), jnp.float32)
    slot = lax.rem(u, 6)
    to_high = [jnp.where((slot < 3) & (slot >= 3 - k), DAMP[k], zero) for k in (1, 2, 3)]
    to_low = [jnp.where((slot >= 3) & (slot < 3 + k), DAMP[k], zero) for k in (1, 2, 3)]
    windows = [(u + 32 - 6 * r) % 32 < 6 for r in range(5)]

    @pl.loop(0, 8)
    def _(t):
        for p in range(5):
            faces = zero
            for r in range(5 if p < 4 else 4):
                faces = jnp.where(windows[r], roll(tile(p * 5 + r, t), 6 * r), faces)
            terms = [roll(faces, 32 - k) * to_high[k - 1] + roll(faces, k - 32) * to_low[k - 1] for k in (1, 2, 3)]
            mb[pl.ds(t % 4 * 128 + t // 4 * 5 + p, 8, stride=16), :] = terms[0] + terms[1] + terms[2]

    pl.semaphore_wait(barrier, 33)

    def pair_rows(ref, j):
        return ref.at[pl.ds(pl.multiple_of(16 * j, 8), 10)]

    for d in NEAR[:-1]:
        peer = device(*d)
        pltpu.make_async_remote_copy(
            pair_rows(mb, pair_at(*d)), rb.at[me, pl.ds(0, 10)], s_1, r_1,
            device_id={"gz": peer}, device_id_type=MESH).start()
    my_pair = pair_at(0, 0, 0)
    pltpu.make_async_copy(pair_rows(mb, my_pair), rb.at[me, pl.ds(0, 10)], r_1).start()
    pl.semaphore_signal(beside, inc=1, device_id={"gz": device(0, 0, 1)}, device_id_type=MESH)

    first = lax.broadcasted_iota(jnp.int32, (8, LANES), 0) < 4
    for f in range(0, FIELDS, 2):
        lo0, lo1 = xp[f, pl.ds(24, 8), :], xp[f + 1, pl.ds(24, 8), :]
        hi0, hi1 = xp[f, pl.ds(64, 8), :], xp[f + 1, pl.ds(64, 8), :]
        xs[0, f // 2] = jnp.where(first, lo0, pltpu.roll(lo1, 4, axis=0))
        xs[1, f // 2] = jnp.where(first, pltpu.roll(hi0, 4, axis=0), hi1)

    send_y = pltpu.make_async_remote_copy(
        xp.at[:, pl.ds(16, 64)], sy, s_y, r_y, device_id={"gy": 1 - gy}, device_id_type=MESH)
    send_y.start()
    send_x = [
        pltpu.make_async_remote_copy(
            xp.at[:, pl.ds(16, 8)], xp.at[:, pl.ds(80, 8)], s_x.at[0], r_x.at[0],
            device_id={"gx": 1 - gx}, device_id_type=MESH),
        pltpu.make_async_remote_copy(
            xp.at[:, pl.ds(72, 8)], xp.at[:, pl.ds(8, 8)], s_x.at[1], r_x.at[1],
            device_id={"gx": 1 - gx}, device_id_type=MESH),
        pltpu.make_async_remote_copy(
            xs, xr, s_x.at[2], r_x.at[2], device_id={"gx": 1 - gx}, device_id_type=MESH),
    ]
    for s in send_x:
        s.start()

    pl.semaphore_wait(beside, 1)
    pl.semaphore_signal(beyond, inc=1, device_id={"gz": device(6, 3, 0)}, device_id_type=MESH)

    load_tab.wait()
    for t in range(8):
        lap[t] = 1.0 + 0.25 * jnp.tanh(tile(0, t))
        total = tile(12, t)
        for f in range(13, 24):
            total = total + tile(f, t)
        lap[8 + t] = lap[t] * (total * (1.0 / 12.0))

    low = [b >= k for k in (1, 2, 3)]
    high = [b < 32 - k for k in (1, 2, 3)]
    left = [lanes >= 32 * k for k in (1, 2, 3)]
    right = [lanes < 128 - 32 * k for k in (1, 2, 3)]

    def plane(f, xg):
        values = [sy[f, pl.ds(xg * 32 + 3, 8, stride=4), :]]
        values += [tile(f, xg * 4 + q) for q in range(4)]
        values += [sy[f, pl.ds(xg * 32, 8, stride=4), :]]
        turned = [[v] + [roll(v, 32 * j) for j in (1, 2, 3)] for v in values]
        sums = []
        for q in range(4):
            v = values[q + 1]
            three = []
            for k in (1, 2, 3):
                plus = jnp.where(right[k - 1], turned[q + 1][4 - k], turned[q + 2][4 - k])
                minus = jnp.where(left[k - 1], turned[q + 1][k], turned[q][k])
                up = jnp.where(high[k - 1], roll(v, -k), 0.0)
                down = jnp.where(low[k - 1], roll(v, k), 0.0)
                three.append((plus + minus) + (up + down))
            sums.append((v, three))
        return sums

    send_y.wait_recv()

    @pl.loop(0, HALF)
    def _(f):
        for xg in range(2):
            us, vs = plane(f, xg), plane(f + HALF, xg)
            for q in range(4):
                t = xg * 4 + q
                lapse, drag = lap[t], lap[8 + t]
                uv, (u1, u2, u3) = us[q]
                vv, (v1, v2, v3) = vs[q]
                damp_u = (2 * DAMP[0]) * uv + DAMP[1] * u1 + DAMP[2] * u2 + DAMP[3] * u3
                damp_v = (2 * DAMP[0]) * vv + DAMP[1] * v1 + DAMP[2] * v2 + DAMP[3] * v3
                laplace = (2 * LAP[0]) * uv + LAP[1] * u1 + LAP[2] * u2
                rt[f, t] = damp_u - 2.0 * lapse * vv
                rt[f + HALF, t] = damp_v + drag * vv - 0.5 * lapse * laplace

    load_base.wait()
    load_accum.wait()
    pltpu.make_async_copy(rb.at[pl.ds(0, 20)], rb.at[pl.ds(0, 20)], r_1).wait()
    pl.semaphore_wait(beyond, 1)
    kind = slot < 3
    my_slot = z // 4 * 32 + my_pair

    def permute(plane):
        for k in range(8):
            g = plane * 8 + k
            below_g, above_g = rb[tab[0, 0, g]], rb[tab[1, 0, g]]
            fb[g] = jnp.concatenate(
                [jnp.where(kind, above_g[h:h + 8], below_g[h:h + 8]) for h in (0, 8)], axis=0)

    def forward(peer):
        @pl.when(peer != me)
        def _():
            pltpu.make_async_remote_copy(
                fb.at[peer, pl.ds(0, 10)], pair_rows(gb, my_slot), s_2, r_2.at[z],
                device_id={"gz": peer}, device_id_type=MESH).start()

    for planes_now in ((0, 1, 2, 3), (4, 5, 6, 7)):
        for plane in planes_now:
            permute(plane)
        for peer in sorted((p * 8 + k for p in planes_now for k in range(8)), key=lambda p: (9 * (p // 8) + (0, 16, 30, 30)[p % 8 // 2] + 10 * (p % 2), p)):
            forward(peer)

    pltpu.make_async_copy(fb.at[me, pl.ds(0, 10)], pair_rows(gb, my_slot), r_2.at[z]).start()

    for s in send_x:
        s.wait_recv()
    for f in range(0, FIELDS, 2):
        hi, lo = xr[0, f // 2], xr[1, f // 2]
        xp[f, pl.ds(88, 8), :] = hi
        xp[f + 1, pl.ds(88, 8), :] = pltpu.roll(hi, 4, axis=0)
        xp[f, pl.ds(0, 8), :] = pltpu.roll(lo, 4, axis=0)
        xp[f + 1, pl.ds(0, 8), :] = lo

    def add(f, t, rate):
        rows = pl.ds(row(t), 8, stride=4)
        q1[f, rows, :] = q1[f, rows, :] + C1 * rate
        q2[f, rows, :] = q2[f, rows, :] + C2 * rate

    @pl.loop(0, HALF)
    def _(f):
        for t in range(8):
            def shifted(field, k):
                return xp[field, pl.ds(16 + row(t) + 4 * k, 8, stride=4), :]

            def three(field):
                return [shifted(field, k) + shifted(field, -k) for k in (1, 2, 3)]

            uv, vv = shifted(f, 0), shifted(f + HALF, 0)
            u1, u2, u3 = three(f)
            v1, v2, v3 = three(f + HALF)
            damp_u = DAMP[0] * uv + DAMP[1] * u1 + DAMP[2] * u2 + DAMP[3] * u3
            damp_v = DAMP[0] * vv + DAMP[1] * v1 + DAMP[2] * v2 + DAMP[3] * v3
            laplace = LAP[0] * uv + LAP[1] * u1 + LAP[2] * u2
            add(f, t, rt[f, t] + damp_u)
            add(f + HALF, t, rt[f + HALF, t] + damp_v - 0.5 * lap[t] * laplace)

    send_y.wait_send()
    for s in send_x:
        s.wait_send()
    pltpu.make_async_copy(mb.at[pl.ds(0, 310)], mb.at[pl.ds(0, 310)], s_1).wait()

    edge = (b < 3) | (b >= 29)
    edge_1, edge_2 = jnp.where(edge, C1, zero), jnp.where(edge, C2, zero)
    next_up = jnp.where((slot == 3) | (slot == 4), ALPHA, zero)
    next_down = jnp.where((slot == 1) | (slot == 2), ALPHA, zero)
    second_up = jnp.where(slot == 3, BETA, zero)
    second_down = jnp.where(slot == 2, BETA, zero)

    sub = lax.broadcasted_iota(jnp.int32, (8, LANES), 0)

    def reached(neighbour, t):
        nz, ny, nx = neighbour // 8, neighbour % 8 // 2, neighbour % 2
        dz, dy = jnp.abs(nz - t), jnp.abs(sub // 2 - ny)
        dx = jnp.abs(sub % 2 - nx)
        return jnp.minimum(dz, 8 - dz) + jnp.minimum(dy, 4 - dy) + dx

    chosen = []
    for t in range(4):
        chosen.append(jnp.where(kind, reached(tab[1, 0, me], t), reached(tab[0, 0, me], t)) <= REACH)

    for t in (1, 5, 0, 4, 2, 6, 3, 7):
        if t < 4:
            for plane in (t, t + 4):
                pltpu.make_async_copy(gb.at[pl.ds(0, 80)], gb.at[pl.ds(0, 80)], r_2.at[plane]).wait()
        packed = []
        for p in range(5):
            start = t % 4 * 128 + t // 4 * 5 + p
            packed.append(jnp.where(
                chosen[t % 4],
                gb[pl.ds(start, 8, stride=16), :],
                gb[pl.ds(512 + start, 8, stride=16), :]))
        half_lapse = -0.5 * lap[t]
        laplaces = [
            roll(v, -1) * next_up + roll(v, 1) * next_down + roll(v, -2) * second_up + roll(v, 2) * second_down
            for v in packed[:3]
        ]
        rows = pl.ds(row(t), 8, stride=4)

        def add_edge(f, rate):
            q1[f, rows, :] = q1[f, rows, :] + edge_1 * rate
            q2[f, rows, :] = q2[f, rows, :] + edge_2 * rate

        for f in range(HALF):
            g = f + HALF
            add_edge(f, roll(packed[f // 5], -6 * (f % 5)))
            add_edge(g, roll(packed[g // 5], -6 * (g % 5)) + half_lapse * roll(laplaces[f // 5], -6 * (f % 5)))

    pltpu.make_async_copy(gb.at[pl.ds(0, 630)], gb.at[pl.ds(0, 630)], s_2).wait()


PIECES = 1


def kernel_b(q1, q2, o1, o2, sems):
    copies = []
    for i in range(PIECES):
        part = pl.ds(i * (FIELDS // PIECES), FIELDS // PIECES)
        copies.append(pltpu.make_async_copy(q1.at[part], o1.at[part], sems.at[0, i]))
        copies.append(pltpu.make_async_copy(q2.at[part], o2.at[part], sems.at[1, i]))
    for c in copies:
        c.start()
    for c in copies:
        c.wait()


def local(state, base, accum, owner):
    shape = state.shape
    f32 = jnp.float32
    rows = (FIELDS, 64, LANES)
    hbm = pl.BlockSpec(memory_space=pltpu.HBM)
    vmem = pl.BlockSpec(memory_space=pltpu.VMEM)
    dma = pltpu.SemaphoreType.DMA
    in_hbm = [pltpu.with_memory_space_constraint(v, pltpu.HBM)
              for v in (state.reshape(rows), base.reshape(rows), accum.reshape(rows), owner)]
    q1, q2 = pl.pallas_call(
        kernel_a,
        out_shape=(pltpu.VMEM(rows, f32), pltpu.VMEM(rows, f32)),
        in_specs=[hbm] * 4,
        out_specs=(vmem, vmem),
        scratch_shapes=[
            pltpu.VMEM((FIELDS, 96, LANES), f32),
            pltpu.VMEM(rows, f32),
            pltpu.VMEM((FIELDS, 8, 8, LANES), f32),
            pltpu.VMEM((16, 8, LANES), f32),
            pltpu.VMEM((512, LANES), f32),
            pltpu.VMEM((64, 16, LANES), f32),
            pltpu.VMEM((64, 16, LANES), f32),
            pltpu.VMEM((1024, LANES), f32),
            pltpu.VMEM((2, 12, 8, LANES), f32),
            pltpu.VMEM((2, 12, 8, LANES), f32),
            pltpu.VMEM((2, 8, LANES), jnp.int32),
            pltpu.SMEM((2, 8, LANES), jnp.int32),
            pltpu.SMEM((64,), jnp.int32),
            dma((4,)), dma, dma, dma, dma((3,)), dma((3,)), dma, dma, dma, dma((8,)),
            pltpu.SemaphoreType.REGULAR, pltpu.SemaphoreType.REGULAR,
        ],
        compiler_params=pltpu.CompilerParams(collective_id=0, has_side_effects=True, vmem_limit_bytes=24 << 20),
    )(*in_hbm)
    o1, o2 = pl.pallas_call(
        kernel_b,
        out_shape=(jax.ShapeDtypeStruct(rows, f32),) * 2,
        in_specs=[vmem, vmem],
        out_specs=(hbm, hbm),
        scratch_shapes=[dma((2, PIECES))],
        compiler_params=pltpu.CompilerParams(vmem_limit_bytes=24 << 20),
    )(q1, q2)
    return o1.reshape(shape), o2.reshape(shape)


def solution(mesh):
    spec = P(None, "gx", ("gy", "gz"), None)
    return jax.shard_map(
        local, mesh=mesh, in_specs=(spec, spec, spec, P()), out_specs=(spec, spec), check_vma=False)
```

```python
import functools

import jax
import jax.numpy as jnp
from jax import lax
from jax.experimental import pallas as pl
from jax.experimental.pallas import tpu as pltpu
from jax.sharding import PartitionSpec as P

MESH = pl.DeviceIdType.MESH
FIELDS, HALF = 24, 12
LANES = 128
C1 = 0.5 * 0.25
C2 = 0.25 / 3.0
DAMP = (-20.0 / 64.0, 15.0 / 64.0, -6.0 / 64.0, 1.0 / 64.0)
LAP = (-30.0 / 12.0, 16.0 / 12.0, -1.0 / 12.0)
ALPHA = LAP[2] / DAMP[3]
BETA = (LAP[1] - LAP[2] * DAMP[2] / DAMP[3]) / DAMP[3]
REACH = 3


def hops(dz, dy, dx):
    return min(dz, 8 - dz) + min(dy, 4 - dy) + dx


NEAR = sorted(
    ((dz, dy, dx) for dz in range(8) for dy in range(4) for dx in range(2) if hops(dz, dy, dx) <= REACH),
    key=lambda d: -hops(*d))


def lane_iota(rows=8):
    return lax.broadcasted_iota(jnp.int32, (rows, LANES), 1)


def roll(v, s):
    s %= LANES
    return v if s == 0 else pltpu.roll(v, s, axis=1)


def kernel_a(state, base, accum, owner_hbm, q1, q2,
             xp, sy, rt, lap, mb, rb, fb, gb, xs, xr, tabv, tab, owner,
             s_in, s_tab, s_y, r_y, s_x, r_x, s_1, r_1, s_2, r_2, beside, beyond):
    gx, gy, me = lax.axis_index("gx"), lax.axis_index("gy"), lax.axis_index("gz")
    z, w = me // 8, lax.rem(me, 8)
    y, x = w // 2, lax.rem(w, 2)

    load_state = pltpu.make_async_copy(state, xp.at[:, pl.ds(16, 64)], s_in.at[0])
    load_base = pltpu.make_async_copy(base, q1, s_in.at[1])
    load_accum = pltpu.make_async_copy(accum, q2, s_in.at[2])
    load_owner = pltpu.make_async_copy(owner_hbm, owner, s_in.at[3])
    load_state.start()
    load_owner.start()

    barrier = pltpu.get_barrier_semaphore()

    zs = [lax.rem(z + d, 8) for d in range(8)]
    ws = [[lax.rem(y + dy, 4) * 2 + lax.rem(x + dx, 2) for dx in range(2)] for dy in range(4)]
    halves = [v // 4 for v in zs[:4]]
    halves += [1 - v for v in halves]
    planes = [lax.rem(z + d, 4) * 8 for d in range(4)]

    def device(dz, dy, dx):
        return zs[dz] * 8 + ws[dy][dx]

    def pair_at(dz, dy, dx):
        across = ws[(dy + 2) % 4][1 - dx] - ws[dy][dx]
        return planes[dz % 4] + ws[dy][dx] + halves[dz] * across

    for d in NEAR[:-1]:
        pl.semaphore_signal(barrier, inc=1, device_id={"gz": device(*d)}, device_id_type=MESH)
    pl.semaphore_signal(barrier, inc=1, device_id={"gy": 1 - gy}, device_id_type=MESH)
    pl.semaphore_signal(barrier, inc=1, device_id={"gx": 1 - gx}, device_id_type=MESH)

    load_owner.wait()
    lanes = lane_iota()
    below = jnp.zeros((8, LANES), jnp.int32)
    above = jnp.zeros((8, LANES), jnp.int32)
    for c in range(64):
        hit = lanes == owner[c]
        below = jnp.where(hit, owner[(c + 63) % 64], below)
        above = jnp.where(hit, owner[(c + 1) % 64], above)
    tabv[0] = below
    tabv[1] = above
    load_tab = pltpu.make_async_copy(tabv, tab, s_tab)

    b = lanes % 32
    u = (lanes + 3) % 32
    load_state.wait()
    load_tab.start()

    def row(t):
        return (t // 4) * 32 + t % 4

    def tile(f, t):
        return xp[f, pl.ds(16 + row(t), 8, stride=4), :]

    zero = jnp.zeros((8, LANES), jnp.float32)
    slot = lax.rem(u, 6)
    to_high = [jnp.where((slot < 3) & (slot >= 3 - k), DAMP[k], zero) for k in (1, 2, 3)]
    to_low = [jnp.where((slot >= 3) & (slot < 3 + k), DAMP[k], zero) for k in (1, 2, 3)]
    windows = [(u + 32 - 6 * r) % 32 < 6 for r in range(5)]

    @pl.loop(0, 8)
    def _(t):
        for p in range(5):
            faces = zero
            for r in range(5 if p < 4 else 4):
                faces = jnp.where(windows[r], roll(tile(p * 5 + r, t), 6 * r), faces)
            terms = [roll(faces, 32 - k) * to_high[k - 1] + roll(faces, k - 32) * to_low[k - 1] for k in (1, 2, 3)]
            mb[pl.ds(t % 4 * 128 + t // 4 * 5 + p, 8, stride=16), :] = terms[0] + terms[1] + terms[2]

    pl.semaphore_wait(barrier, 33)

    def pair_rows(ref, j):
        return ref.at[pl.ds(pl.multiple_of(16 * j, 8), 10)]

    for d in NEAR[:-1]:
        peer = device(*d)
        pltpu.make_async_remote_copy(
            pair_rows(mb, pair_at(*d)), rb.at[me, pl.ds(0, 10)], s_1, r_1,
            device_id={"gz": peer}, device_id_type=MESH).start()
    my_pair = pair_at(0, 0, 0)
    pltpu.make_async_copy(pair_rows(mb, my_pair), rb.at[me, pl.ds(0, 10)], r_1).start()
    pl.semaphore_signal(beside, inc=1, device_id={"gz": device(0, 0, 1)}, device_id_type=MESH)

    first = lax.broadcasted_iota(jnp.int32, (8, LANES), 0) < 4
    for f in range(0, FIELDS, 2):
        lo0, lo1 = xp[f, pl.ds(24, 8), :], xp[f + 1, pl.ds(24, 8), :]
        hi0, hi1 = xp[f, pl.ds(64, 8), :], xp[f + 1, pl.ds(64, 8), :]
        xs[0, f // 2] = jnp.where(first, lo0, pltpu.roll(lo1, 4, axis=0))
        xs[1, f // 2] = jnp.where(first, pltpu.roll(hi0, 4, axis=0), hi1)

    send_y = pltpu.make_async_remote_copy(
        xp.at[:, pl.ds(16, 64)], sy, s_y, r_y, device_id={"gy": 1 - gy}, device_id_type=MESH)
    send_x = [
        pltpu.make_async_remote_copy(
            xp.at[:, pl.ds(16, 8)], xp.at[:, pl.ds(80, 8)], s_x.at[0], r_x.at[0],
            device_id={"gx": 1 - gx}, device_id_type=MESH),
        pltpu.make_async_remote_copy(
            xp.at[:, pl.ds(72, 8)], xp.at[:, pl.ds(8, 8)], s_x.at[1], r_x.at[1],
            device_id={"gx": 1 - gx}, device_id_type=MESH),
        pltpu.make_async_remote_copy(
            xs, xr, s_x.at[2], r_x.at[2], device_id={"gx": 1 - gx}, device_id_type=MESH),
    ]
    for s in send_x:
        s.start()
    send_y.start()

    load_base.start()
    load_accum.start()

    pl.semaphore_wait(beside, 1)
    pl.semaphore_signal(beyond, inc=1, device_id={"gz": device(6, 3, 0)}, device_id_type=MESH)

    load_tab.wait()
    for t in range(8):
        lap[t] = 1.0 + 0.25 * jnp.tanh(tile(0, t))
        total = tile(12, t)
        for f in range(13, 24):
            total = total + tile(f, t)
        lap[8 + t] = lap[t] * (total * (1.0 / 12.0))

    low = [b >= k for k in (1, 2, 3)]
    high = [b < 32 - k for k in (1, 2, 3)]
    left = [lanes >= 32 * k for k in (1, 2, 3)]
    right = [lanes < 128 - 32 * k for k in (1, 2, 3)]

    def plane(f, xg):
        values = [sy[f, pl.ds(xg * 32 + 3, 8, stride=4), :]]
        values += [tile(f, xg * 4 + q) for q in range(4)]
        values += [sy[f, pl.ds(xg * 32, 8, stride=4), :]]
        turned = [[v] + [roll(v, 32 * j) for j in (1, 2, 3)] for v in values]
        sums = []
        for q in range(4):
            v = values[q + 1]
            three = []
            for k in (1, 2, 3):
                plus = jnp.where(right[k - 1], turned[q + 1][4 - k], turned[q + 2][4 - k])
                minus = jnp.where(left[k - 1], turned[q + 1][k], turned[q][k])
                up = jnp.where(high[k - 1], roll(v, -k), 0.0)
                down = jnp.where(low[k - 1], roll(v, k), 0.0)
                three.append((plus + minus) + (up + down))
            sums.append((v, three))
        return sums

    send_y.wait_recv()

    @pl.loop(0, HALF)
    def _(f):
        for xg in range(2):
            us, vs = plane(f, xg), plane(f + HALF, xg)
            for q in range(4):
                t = xg * 4 + q
                lapse, drag = lap[t], lap[8 + t]
                uv, (u1, u2, u3) = us[q]
                vv, (v1, v2, v3) = vs[q]
                damp_u = (2 * DAMP[0]) * uv + DAMP[1] * u1 + DAMP[2] * u2 + DAMP[3] * u3
                damp_v = (2 * DAMP[0]) * vv + DAMP[1] * v1 + DAMP[2] * v2 + DAMP[3] * v3
                laplace = (2 * LAP[0]) * uv + LAP[1] * u1 + LAP[2] * u2
                rt[f, t] = damp_u - 2.0 * lapse * vv
                rt[f + HALF, t] = damp_v + drag * vv - 0.5 * lapse * laplace

    load_base.wait()
    load_accum.wait()
    pltpu.make_async_copy(rb.at[pl.ds(0, 20)], rb.at[pl.ds(0, 20)], r_1).wait()
    pl.semaphore_wait(beyond, 1)
    kind = slot < 3
    my_slot = z // 4 * 32 + my_pair

    def permute(plane):
        for k in range(8):
            g = plane * 8 + k
            below_g, above_g = rb[tab[0, 0, g]], rb[tab[1, 0, g]]
            fb[g] = jnp.concatenate(
                [jnp.where(kind, above_g[h:h + 8], below_g[h:h + 8]) for h in (0, 8)], axis=0)

    def forward(peer):
        @pl.when(peer != me)
        def _():
            pltpu.make_async_remote_copy(
                fb.at[peer, pl.ds(0, 10)], pair_rows(gb, my_slot), s_2, r_2.at[z],
                device_id={"gz": peer}, device_id_type=MESH).start()

    for planes_now in ((0, 1, 2, 3), (4, 5, 6, 7)):
        for plane in planes_now:
            permute(plane)
        for peer in sorted((p * 8 + k for p in planes_now for k in range(8)), key=lambda p: (9 * (p // 8) + (0, 16, 30, 30)[p % 8 // 2] + 10 * (p % 2), p)):
            forward(peer)

    pltpu.make_async_copy(fb.at[me, pl.ds(0, 10)], pair_rows(gb, my_slot), r_2.at[z]).start()

    for s in send_x:
        s.wait_recv()
    for f in range(0, FIELDS, 2):
        hi, lo = xr[0, f // 2], xr[1, f // 2]
        xp[f, pl.ds(88, 8), :] = hi
        xp[f + 1, pl.ds(88, 8), :] = pltpu.roll(hi, 4, axis=0)
        xp[f, pl.ds(0, 8), :] = pltpu.roll(lo, 4, axis=0)
        xp[f + 1, pl.ds(0, 8), :] = lo

    def add(f, t, rate):
        rows = pl.ds(row(t), 8, stride=4)
        q1[f, rows, :] = q1[f, rows, :] + C1 * rate
        q2[f, rows, :] = q2[f, rows, :] + C2 * rate

    @pl.loop(0, HALF)
    def _(f):
        for t in range(8):
            def shifted(field, k):
                return xp[field, pl.ds(16 + row(t) + 4 * k, 8, stride=4), :]

            def three(field):
                return [shifted(field, k) + shifted(field, -k) for k in (1, 2, 3)]

            uv, vv = shifted(f, 0), shifted(f + HALF, 0)
            u1, u2, u3 = three(f)
            v1, v2, v3 = three(f + HALF)
            damp_u = DAMP[0] * uv + DAMP[1] * u1 + DAMP[2] * u2 + DAMP[3] * u3
            damp_v = DAMP[0] * vv + DAMP[1] * v1 + DAMP[2] * v2 + DAMP[3] * v3
            laplace = LAP[0] * uv + LAP[1] * u1 + LAP[2] * u2
            add(f, t, rt[f, t] + damp_u)
            add(f + HALF, t, rt[f + HALF, t] + damp_v - 0.5 * lap[t] * laplace)

    send_y.wait_send()
    for s in send_x:
        s.wait_send()
    pltpu.make_async_copy(mb.at[pl.ds(0, 310)], mb.at[pl.ds(0, 310)], s_1).wait()

    edge = (b < 3) | (b >= 29)
    edge_1, edge_2 = jnp.where(edge, C1, zero), jnp.where(edge, C2, zero)
    next_up = jnp.where((slot == 3) | (slot == 4), ALPHA, zero)
    next_down = jnp.where((slot == 1) | (slot == 2), ALPHA, zero)
    second_up = jnp.where(slot == 3, BETA, zero)
    second_down = jnp.where(slot == 2, BETA, zero)

    sub = lax.broadcasted_iota(jnp.int32, (8, LANES), 0)

    def reached(neighbour, t):
        nz, ny, nx = neighbour // 8, neighbour % 8 // 2, neighbour % 2
        dz, dy = jnp.abs(nz - t), jnp.abs(sub // 2 - ny)
        dx = jnp.abs(sub % 2 - nx)
        return jnp.minimum(dz, 8 - dz) + jnp.minimum(dy, 4 - dy) + dx

    chosen = []
    for t in range(4):
        chosen.append(jnp.where(kind, reached(tab[1, 0, me], t), reached(tab[0, 0, me], t)) <= REACH)

    for t in (1, 5, 0, 4, 2, 6, 3, 7):
        if t < 4:
            for plane in (t, t + 4):
                pltpu.make_async_copy(gb.at[pl.ds(0, 80)], gb.at[pl.ds(0, 80)], r_2.at[plane]).wait()
        packed = []
        for p in range(5):
            start = t % 4 * 128 + t // 4 * 5 + p
            packed.append(jnp.where(
                chosen[t % 4],
                gb[pl.ds(start, 8, stride=16), :],
                gb[pl.ds(512 + start, 8, stride=16), :]))
        half_lapse = -0.5 * lap[t]
        laplaces = [
            roll(v, -1) * next_up + roll(v, 1) * next_down + roll(v, -2) * second_up + roll(v, 2) * second_down
            for v in packed[:3]
        ]
        rows = pl.ds(row(t), 8, stride=4)

        def add_edge(f, rate):
            q1[f, rows, :] = q1[f, rows, :] + edge_1 * rate
            q2[f, rows, :] = q2[f, rows, :] + edge_2 * rate

        for f in range(HALF):
            g = f + HALF
            add_edge(f, roll(packed[f // 5], -6 * (f % 5)))
            add_edge(g, roll(packed[g // 5], -6 * (g % 5)) + half_lapse * roll(laplaces[f // 5], -6 * (f % 5)))

    pltpu.make_async_copy(gb.at[pl.ds(0, 630)], gb.at[pl.ds(0, 630)], s_2).wait()


PIECES = 1


def kernel_b(q1, q2, o1, o2, sems):
    copies = []
    for i in range(PIECES):
        part = pl.ds(i * (FIELDS // PIECES), FIELDS // PIECES)
        copies.append(pltpu.make_async_copy(q1.at[part], o1.at[part], sems.at[0, i]))
        copies.append(pltpu.make_async_copy(q2.at[part], o2.at[part], sems.at[1, i]))
    for c in copies:
        c.start()
    for c in copies:
        c.wait()


def local(state, base, accum, owner):
    shape = state.shape
    f32 = jnp.float32
    rows = (FIELDS, 64, LANES)
    hbm = pl.BlockSpec(memory_space=pltpu.HBM)
    vmem = pl.BlockSpec(memory_space=pltpu.VMEM)
    dma = pltpu.SemaphoreType.DMA
    in_hbm = [pltpu.with_memory_space_constraint(v, pltpu.HBM)
              for v in (state.reshape(rows), base.reshape(rows), accum.reshape(rows), owner)]
    q1, q2 = pl.pallas_call(
        kernel_a,
        out_shape=(pltpu.VMEM(rows, f32), pltpu.VMEM(rows, f32)),
        in_specs=[hbm] * 4,
        out_specs=(vmem, vmem),
        scratch_shapes=[
            pltpu.VMEM((FIELDS, 96, LANES), f32),
            pltpu.VMEM(rows, f32),
            pltpu.VMEM((FIELDS, 8, 8, LANES), f32),
            pltpu.VMEM((16, 8, LANES), f32),
            pltpu.VMEM((512, LANES), f32),
            pltpu.VMEM((64, 16, LANES), f32),
            pltpu.VMEM((64, 16, LANES), f32),
            pltpu.VMEM((1024, LANES), f32),
            pltpu.VMEM((2, 12, 8, LANES), f32),
            pltpu.VMEM((2, 12, 8, LANES), f32),
            pltpu.VMEM((2, 8, LANES), jnp.int32),
            pltpu.SMEM((2, 8, LANES), jnp.int32),
            pltpu.SMEM((64,), jnp.int32),
            dma((4,)), dma, dma, dma, dma((3,)), dma((3,)), dma, dma, dma, dma((8,)),
            pltpu.SemaphoreType.REGULAR, pltpu.SemaphoreType.REGULAR,
        ],
        compiler_params=pltpu.CompilerParams(collective_id=0, has_side_effects=True, vmem_limit_bytes=24 << 20),
    )(*in_hbm)
    o1, o2 = pl.pallas_call(
        kernel_b,
        out_shape=(jax.ShapeDtypeStruct(rows, f32),) * 2,
        in_specs=[vmem, vmem],
        out_specs=(hbm, hbm),
        scratch_shapes=[dma((2, PIECES))],
        compiler_params=pltpu.CompilerParams(vmem_limit_bytes=24 << 20),
    )(q1, q2)
    return o1.reshape(shape), o2.reshape(shape)


def solution(mesh):
    spec = P(None, "gx", ("gy", "gz"), None)
    return jax.shard_map(
        local, mesh=mesh, in_specs=(spec, spec, spec, P()), out_specs=(spec, spec), check_vma=False)
```
